128 devices in a mesh: tm: 4 (over x), space: 32 (over z, y, core).
Axes of the slice: x: 4, y: 4, z: 4, core: 2. Of those that a mesh axis runs over, the one named last changes fastest.
Arguments:
- source: float32 [32, 2048, 1024], P('tm', 'space'), may hold values from -6 to 6
- guess: float32 [32, 2048, 1024], P('tm', 'space'), may hold values from -6 to 6
- start_state: float32 [2048, 1024], P('space'), may hold values from -6 to 6
- conduct: float32 [2048, 1024], P('space'), may hold values from 0.5 to 4
Outputs:
- solution_field: float32 [32, 2048, 1024], P('tm', 'space')
- residual: float32 [32, 2048, 1024], P('tm', 'space')
The draws below stay inside these ranges and needn't reach their ends.
All inputs are finite; a program needn't handle non-finite values.
Results may differ from the reference program's by a relative error of at most 0.00002.
Values sent between devices are 32-bit elements; how exact they have to be, the bound alone decides.
A program may use at most 64 MiB of HBM per device.

```python
import math
import jax
import jax.numpy as jnp

COLS = 1024
NT = 32
NR = 2048


def levels(rng, extent, cuts, smallest, high):
    loudness = 1.0
    for position, blocks in cuts:
        heights = jax.random.uniform(jax.random.fold_in(jax.random.fold_in(rng, 6), position), (blocks,), jnp.float32, smallest / len(cuts), high / len(cuts))
        loudness = loudness * jnp.repeat(jnp.exp(heights), extent[position] // blocks).reshape((-1,) + (1,) * (len(extent) - 1 - position))
    return loudness


def normal_values(rng, extent, width, reach, pieces=(), kind=jnp.bfloat16):
    entries = width * jax.random.normal(rng, extent, jnp.float32)
    if pieces:
        entries = entries * levels(rng, extent, pieces, -0.22, 0.18)
    return jnp.clip(entries, -reach, reach).astype(kind)


def setup_inputs(seed: int = 0) -> dict:
    key_list = jax.random.split(jax.random.key(seed), 5)
    source = normal_values(key_list[0], (NT, NR, COLS), 1.0, 6.0, ((0, 4), (1, 32)), jnp.float32)
    guess = normal_values(key_list[1], (NT, NR, COLS), 1.0, 6.0, ((0, 4), (1, 32)), jnp.float32)
    start_state = normal_values(key_list[2], (NR, COLS), 1.0, 6.0, ((0, 32),), jnp.float32)
    conduct = jnp.clip(jnp.exp(math.log(4.0) - 2.0794415 * jax.random.uniform(key_list[3], (NR, COLS), jnp.float32) ** levels(key_list[3], (NR, COLS), ((0, 32),), -0.2, 0.2)), 0.5, 4.0)
    return dict(source=source, guess=guess, start_state=start_state, conduct=conduct)


damping = 0.8


def apply_operator(field, conduct):
    padded = jnp.pad(field, ((0, 0), (1, 1), (1, 1)))
    beside = padded[:, 2:, 1:-1] + padded[:, :-2, 1:-1] + padded[:, 1:-1, 2:] + padded[:, 1:-1, :-2]
    return field + conduct * (4.0 * field - beside)


def approx_inverse(resid, conduct):
    diagonal = 1.0 + 4.0 * conduct
    first_sweep = resid / diagonal
    return first_sweep + (resid - apply_operator(first_sweep, conduct)) / diagonal


def fine_residual(field, before, source, conduct):
    earlier = jnp.concatenate([before[None], field[:-1]], axis=0)
    return source + earlier - apply_operator(field, conduct)


def shifted(coarse):
    return jnp.concatenate([jnp.zeros_like(coarse[:1]), coarse[:-1]], axis=0)


def reference(source, guess, start_state, conduct):
    resid0 = fine_residual(guess, start_state, source, conduct)
    smooth1 = guess + damping * approx_inverse(resid0, conduct)
    resid1 = fine_residual(smooth1, start_state, source, conduct)
    half_steps = source.shape[0] // 2
    pairs = resid1.reshape(half_steps, 2, source.shape[1], source.shape[2])
    restricted = pairs[:, 0] + pairs[:, 1]
    coarse_cond = 2.0 * conduct
    correction = damping * approx_inverse(restricted, coarse_cond)
    for sweep in range(2):
        defect = restricted + shifted(correction) - apply_operator(correction, coarse_cond)
        correction = correction + damping * approx_inverse(defect, coarse_cond)
    even_steps = 0.5 * (shifted(correction) + correction)
    fine_corr = jnp.stack([even_steps, correction], axis=1).reshape(source.shape)
    smooth2 = smooth1 + fine_corr
    resid2 = fine_residual(smooth2, start_state, source, conduct)
    smooth3 = smooth2 + damping * approx_inverse(resid2, conduct)
    resid3 = fine_residual(smooth3, start_state, source, conduct)
    return smooth3, resid3
```

```python
import functools

import jax
import jax.numpy as jnp
from jax import lax
from jax.experimental import pallas as pl
from jax.experimental.pallas import tpu as pltpu
from jax.sharding import PartitionSpec as P

damping = 0.8
MESH = pl.DeviceIdType.MESH
LANES = 128
HALO = 8
TOP = 16
CHUNK = 16


def cycle_kernel(
    steps,
    rows,
    blocks,
    source_hbm,
    guess_hbm,
    start_hbm,
    cond_hbm,
    u3,
    res,
    src,
    gue,
    u1,
    u2,
    e0,
    e1,
    e2,
    rhs,
    tmp,
    coef,
    load_sem,
    xs,
    xr,
    hs,
    hr,
):
    half = steps // 2
    end = TOP + rows
    tm, sp = lax.axis_index("tm"), lax.axis_index("space")
    n_tm, n_sp = lax.axis_size("tm"), lax.axis_size("space")
    first, last = tm == 0, tm == n_tm - 1
    top, bottom = sp == 0, sp == n_sp - 1
    COND, INV, W, INVK, WK = range(5)

    def load(group, hbm, lead, buf, at, count):
        out = []
        for k in range(blocks):
            cols = pl.ds(k * LANES, LANES)
            view = hbm.at[:, cols] if lead is None else hbm.at[pl.ds(lead, count), :, cols]
            dst = buf.at[at, k, pl.ds(TOP, rows), :] if lead is None else buf.at[pl.ds(at, count), k, pl.ds(TOP, rows), :]
            out.append(pltpu.make_async_copy(view, dst, load_sem.at[group, k]))
        return out

    loads = {
        "g_last": load(0, guess_hbm, steps - 2, gue, steps - 1, 2),
        "cond": load(1, cond_hbm, None, coef, COND, 1),
        "s_last": load(2, source_hbm, steps - 2, src, steps - 2, 2),
        "g_rest": load(3, guess_hbm, 0, gue, 1, steps - 2),
        "s_rest": load(4, source_hbm, 0, src, 0, steps - 2),
    }
    starts = [load(5 + i, start_hbm, None, buf, 0, 1) for i, buf in enumerate((gue, u1, u3))]

    def start(copies):
        for c in copies:
            c.start()

    def wait(copies):
        for c in copies:
            c.wait()

    for name in ("g_last", "cond", "s_last", "g_rest", "s_rest"):
        start(loads[name])

    @pl.when(first)
    def _():
        for copies in starts:
            start(copies)

    barrier = pltpu.get_barrier_semaphore()

    def greet(cond, axis, index):
        @pl.when(cond)
        def _():
            pl.semaphore_signal(barrier, inc=1, device_id={axis: index}, device_id_type=MESH)

    greet(~first, "tm", tm - 1)
    greet(~last, "tm", tm + 1)
    greet(~top, "space", sp - 1)
    greet(~bottom, "space", sp + 1)
    one = jnp.int32(1)
    zero = jnp.int32(0)
    peers = (
        jnp.where(first, zero, one)
        + jnp.where(last, zero, one)
        + jnp.where(top, zero, one)
        + jnp.where(bottom, zero, one)
    )
    pl.semaphore_wait(barrier, peers)

    own = pl.ds(TOP, rows)

    def x_copy(i, buf, plane):
        return pltpu.make_async_remote_copy(
            src_ref=buf.at[plane, :, own, :],
            dst_ref=buf.at[0, :, own, :],
            send_sem=xs.at[i],
            recv_sem=xr.at[i],
            device_id={"tm": tm + 1},
            device_id_type=MESH,
        )

    x_plan = [(gue, steps), (u1, steps), (e0, half), (e1, half), (e2, half), (u3, steps)]

    def x_send(i):
        @pl.when(~last)
        def _():
            x_copy(i, *x_plan[i]).start()

    def x_wait(i):
        @pl.when(~first)
        def _():
            x_copy(i, *x_plan[i]).wait_recv()

        if i in (0, 1, 5):

            @pl.when(first)
            def _():
                wait(starts[(0, 1, 5).index(i)])

    h_plan = [
        (gue, steps - 1, 2),
        (src, steps - 2, 2),
        (coef, COND, 1),
        (gue, 1, steps - 2),
        (src, 0, steps - 2),
        (gue, 0, 1),
        (u1, 0, 1),
        (e0, 0, 1),
        (e1, 0, 1),
        (e2, 0, 1),
        (e2, half - 1, 2),
        (e2, 2, half - 3),
        (e2, 1, 1),
    ]

    def down_copy(i):
        buf, plane, count = h_plan[i]
        return pltpu.make_async_remote_copy(
            src_ref=buf.at[pl.ds(plane, count), :, pl.ds(end - HALO, HALO), :],
            dst_ref=buf.at[pl.ds(plane, count), :, pl.ds(TOP - HALO, HALO), :],
            send_sem=hs.at[i, 0],
            recv_sem=hr.at[i, 0],
            device_id={"space": sp + 1},
            device_id_type=MESH,
        )

    def up_copy(i):
        buf, plane, count = h_plan[i]
        return pltpu.make_async_remote_copy(
            src_ref=buf.at[pl.ds(plane, count), :, pl.ds(TOP, HALO), :],
            dst_ref=buf.at[pl.ds(plane, count), :, pl.ds(end, HALO), :],
            send_sem=hs.at[i, 1],
            recv_sem=hr.at[i, 1],
            device_id={"space": sp - 1},
            device_id_type=MESH,
        )

    def h_send(*which):
        @pl.when(~bottom)
        def _():
            for i in which:
                down_copy(i).start()

        @pl.when(~top)
        def _():
            for i in which:
                up_copy(i).start()

    def h_wait(*which):
        @pl.when(~top)
        def _():
            for i in which:
                down_copy(i).wait_recv()

        @pl.when(~bottom)
        def _():
            for i in which:
                up_copy(i).wait_recv()

    def at(buf, n, r):
        return buf[n, :, pl.ds(r, CHUNK), :]

    def put(buf, n, r, value):
        buf[n, :, pl.ds(r, CHUNK), :] = value

    def sideways(v):
        lane = lax.broadcasted_iota(jnp.int32, v.shape, 2)
        edge = jnp.zeros((1,) + v.shape[1:], jnp.float32)
        fwd = pltpu.roll(v, 1, 2)
        bwd = pltpu.roll(v, LANES - 1, 2)
        left = jnp.where(lane == 0, jnp.concatenate([edge, fwd[:-1]], axis=0), fwd)
        right = jnp.where(lane == LANES - 1, jnp.concatenate([bwd[1:], edge], axis=0), bwd)
        return left + right

    def with_sum(buf, n, r):
        v = at(buf, n, r)
        return v, (at(buf, n, r - 1) + at(buf, n, r + 1)) + sideways(v)

    def over_rows(low, high, body):
        count = (high - low) // CHUNK

        def step(i, carry):
            body(low + i * CHUNK)
            return carry

        lax.fori_loop(0, count, step, 0, unroll=True)

    def over_planes(low, high, body):
        if high - low == 1:
            body(low)
        else:

            def step(i, carry):
                body(i)
                return carry

            lax.fori_loop(low, high, step, 0)

    wide = (TOP - HALO, end + HALO)

    def fine_smooth(frm, to, low, high):
        def first_pass(n):
            def chunk(r):
                v, s = with_sum(frm, n + 1, r)
                rest = at(src, n, r) + at(frm, n, r)
                put(tmp, n, r, damping * (at(coef, INV, r) * rest + at(coef, W, r) * s - v))

            over_rows(*wide, chunk)

        def second_pass(n):
            def chunk(r):
                v, s = with_sum(tmp, n, r)
                put(to, n + 1, r, at(frm, n + 1, r) + (v + at(coef, W, r) * s))

            over_rows(*wide, chunk)

        over_planes(low, high, first_pass)
        over_planes(low, high, second_pass)

    def restrict(m):
        def chunk(r):
            a, sa = at(u1, 2 * m + 1, r), at(u1, 2 * m + 1, r - 1) + at(u1, 2 * m + 1, r + 1)
            b, sb = at(u1, 2 * m + 2, r), at(u1, 2 * m + 2, r - 1) + at(u1, 2 * m + 2, r + 1)
            pair = a + b
            around = (sa + sb) + sideways(pair)
            total = at(src, 2 * m, r) + at(src, 2 * m + 1, r) + (at(u1, 2 * m, r) - b)
            total = total - at(coef, COND, r) * (4.0 * pair - around)
            put(rhs, m, r, at(coef, INVK, r) * total)

        over_rows(*wide, chunk)

    def coarse_first(m):
        def chunk(r):
            v, s = with_sum(rhs, m, r)
            put(e0, m + 1, r, damping * (v + at(coef, WK, r) * s))

        over_rows(*wide, chunk)

    def coarse_sweep(frm, to, m, slot):
        def first_pass(r):
            v, s = with_sum(frm, m + 1, r)
            rest = at(rhs, m, r) + at(coef, INVK, r) * at(frm, m, r)
            put(tmp, slot, r, damping * (rest + at(coef, WK, r) * s - v))

        def second_pass(r):
            v, s = with_sum(tmp, slot, r)
            put(to, m + 1, r, at(frm, m + 1, r) + (v + at(coef, WK, r) * s))

        over_rows(*wide, first_pass)
        over_rows(*((TOP, end) if to is e2 else wide), second_pass)

    def prolong_odd(m):
        over_rows(*wide, lambda r: put(u2, 2 * m + 2, r, at(u1, 2 * m + 2, r) + at(e2, m + 1, r)))

    def prolong_even(m):
        over_rows(
            *wide,
            lambda r: put(u2, 2 * m + 1, r, at(u1, 2 * m + 1, r) + 0.5 * (at(e2, m, r) + at(e2, m + 1, r))),
        )

    def last_residual(n):
        def chunk(r):
            v, s = with_sum(u3, n + 1, r)
            rest = at(src, n, r) + (at(u3, n, r) - v)
            res[n, :, pl.ds(r - TOP, CHUNK), :] = rest - at(coef, COND, r) * (4.0 * v - s)

        over_rows(TOP, end, chunk)

    def clear(low):
        zeros = jnp.zeros((blocks, HALO, LANES), jnp.float32)

        def planes(buf, a, b):
            for n in range(a, b):
                buf[n, :, pl.ds(low, HALO), :] = zeros

        planes(gue, 0, steps + 1)
        planes(src, 0, steps)
        planes(coef, COND, COND + 1)
        for buf in (u1, e0, e1):
            planes(buf, 0, 1)
        planes(e2, 0, half + 1)

    @pl.when(top)
    def _():
        clear(TOP - HALO)

    @pl.when(bottom)
    def _():
        clear(end)

    @pl.when(first)
    def _():
        for buf in (e0, e1, e2):
            buf[0, :, pl.ds(TOP, rows), :] = jnp.zeros((blocks, rows, LANES), jnp.float32)

    wait(loads["g_last"])
    x_send(0)
    h_send(0)
    wait(loads["cond"])
    wait(loads["s_last"])
    h_send(2, 1)
    wait(loads["g_rest"])
    wait(loads["s_rest"])
    h_send(3, 4)

    h_wait(2)

    def coefficients(r):
        c = at(coef, COND, r)
        inv = 1.0 / (1.0 + 4.0 * c)
        invk = 1.0 / (1.0 + 8.0 * c)
        put(coef, INV, r, inv)
        put(coef, W, r, c * inv)
        put(coef, INVK, r, invk)
        put(coef, WK, r, (2.0 * c) * invk)

    over_rows(*wide, coefficients)
    h_wait(0, 1)
    fine_smooth(gue, u1, steps - 1, steps)
    x_send(1)
    h_wait(3, 4)
    fine_smooth(gue, u1, 1, steps - 1)
    over_planes(1, half, restrict)
    over_planes(half - 1, half, coarse_first)
    x_send(2)
    over_planes(1, half - 1, coarse_first)
    coarse_sweep(e0, e1, half - 1, 0)
    x_send(3)
    over_planes(2, half - 1, lambda m: coarse_sweep(e0, e1, m, 1))
    coarse_sweep(e1, e2, half - 1, 2)
    x_send(4)

    x_wait(0)
    h_send(5)
    h_wait(5)
    fine_smooth(gue, u1, 0, 1)

    x_wait(1)
    h_send(6)
    h_wait(6)
    restrict(0)
    coarse_first(0)
    coarse_sweep(e0, e1, 1, 3)
    coarse_sweep(e1, e2, 2, 4)
    h_send(10)
    h_wait(10)
    prolong_odd(half - 1)
    prolong_even(half - 1)
    fine_smooth(u2, u3, steps - 1, steps)
    x_send(5)
    prolong_odd(half - 2)
    fine_smooth(u2, u3, steps - 2, steps - 1)
    last_residual(steps - 1)

    x_wait(2)
    h_send(7)
    h_wait(7)
    coarse_sweep(e0, e1, 0, 5)
    coarse_sweep(e1, e2, 1, 6)
    h_send(11)
    h_wait(11)
    prolong_even(half - 2)
    prolong_odd(half - 3)
    fine_smooth(u2, u3, steps - 4, steps - 2)
    over_planes(steps - 3, steps - 1, last_residual)

    x_wait(3)
    h_send(8)
    h_wait(8)
    coarse_sweep(e1, e2, 0, 7)
    h_send(12)
    h_wait(12)
    prolong_even(1)
    prolong_odd(0)
    fine_smooth(u2, u3, 2, steps - 4)
    over_planes(3, steps - 3, last_residual)

    x_wait(4)
    h_send(9)
    h_wait(9)
    over_rows(*wide, lambda r: put(u2, 0, r, at(u1, 0, r) + at(e2, 0, r)))
    prolong_even(0)
    fine_smooth(u2, u3, 0, 2)
    over_planes(1, 3, last_residual)

    x_wait(5)
    last_residual(0)

    @pl.when(~last)
    def _():
        for i in range(len(x_plan)):
            x_copy(i, *x_plan[i]).wait_send()

    @pl.when(~bottom)
    def _():
        for i in range(len(h_plan)):
            down_copy(i).wait_send()

    @pl.when(~top)
    def _():
        for i in range(len(h_plan)):
            up_copy(i).wait_send()


def store_kernel(steps, rows, blocks, u3, res, field_out, res_out, sem):
    copies = []
    for k in range(blocks):
        cols = pl.ds(k * LANES, LANES)
        copies.append(
            pltpu.make_async_copy(
                u3.at[pl.ds(1, steps), k, pl.ds(TOP, rows), :], field_out.at[:, :, cols], sem.at[0, k]
            )
        )
        copies.append(pltpu.make_async_copy(res.at[:, k, :, :], res_out.at[:, :, cols], sem.at[1, k]))
    for c in copies:
        c.start()
    for c in copies:
        c.wait()


def shards(source, guess, start_state, conduct):
    steps, rows, cols = source.shape
    blocks = cols // LANES
    half = steps // 2
    tall = rows + 2 * TOP
    f32 = jnp.float32
    hbm = pl.BlockSpec(memory_space=pltpu.HBM)
    vmem = pl.BlockSpec(memory_space=pltpu.VMEM)

    def planes(n):
        return pltpu.VMEM((n, blocks, tall, LANES), f32)

    u3, res = pl.pallas_call(
        functools.partial(cycle_kernel, steps, rows, blocks),
        out_shape=(
            jax.ShapeDtypeStruct((steps + 1, blocks, tall, LANES), f32),
            jax.ShapeDtypeStruct((steps, blocks, rows, LANES), f32),
        ),
        in_specs=[hbm] * 4,
        out_specs=(vmem, vmem),
        scratch_shapes=[
            planes(steps),
            planes(steps + 1),
            planes(steps + 1),
            planes(steps + 1),
            planes(half + 1),
            planes(half + 1),
            planes(half + 1),
            planes(half),
            planes(steps),
            planes(5),
            pltpu.SemaphoreType.DMA((8, blocks)),
            pltpu.SemaphoreType.DMA((6,)),
            pltpu.SemaphoreType.DMA((6,)),
            pltpu.SemaphoreType.DMA((13, 2)),
            pltpu.SemaphoreType.DMA((13, 2)),
        ],
        compiler_params=pltpu.CompilerParams(
            collective_id=0, has_side_effects=True, vmem_limit_bytes=44 * 1024 * 1024
        ),
        name="cycle",
    )(*(pltpu.with_memory_space_constraint(a, pltpu.HBM) for a in (source, guess, start_state, conduct)))
    return pl.pallas_call(
        functools.partial(store_kernel, steps, rows, blocks),
        out_shape=(jax.ShapeDtypeStruct(source.shape, f32), jax.ShapeDtypeStruct(source.shape, f32)),
        in_specs=[vmem, vmem],
        out_specs=(hbm, hbm),
        scratch_shapes=[pltpu.SemaphoreType.DMA((2, blocks))],
        compiler_params=pltpu.CompilerParams(vmem_limit_bytes=16 * 1024 * 1024),
        name="store",
    )(u3, res)


def solution(mesh):
    return jax.shard_map(
        shards,
        mesh=mesh,
        in_specs=(
            P("tm", "space", None),
            P("tm", "space", None),
            P("space", None),
            P("space", None),
        ),
        out_specs=(P("tm", "space", None), P("tm", "space", None)),
        check_vma=False,
    )
```

```python
import functools

import jax
import jax.numpy as jnp
from jax import lax
from jax.experimental import pallas as pl
from jax.experimental.pallas import tpu as pltpu
from jax.sharding import PartitionSpec as P

damping = 0.8
MESH = pl.DeviceIdType.MESH
LANES = 128
HALO = 8
TOP = 16
CHUNK = 16


def cycle_kernel(
    steps,
    rows,
    blocks,
    source_hbm,
    guess_hbm,
    start_hbm,
    cond_hbm,
    u3,
    res,
    src,
    gue,
    u1,
    u2,
    e0,
    e1,
    e2,
    rhs,
    tmp,
    coef,
    load_sem,
    xs,
    xr,
    hs,
    hr,
):
    half = steps // 2
    end = TOP + rows
    tm, sp = lax.axis_index("tm"), lax.axis_index("space")
    n_tm, n_sp = lax.axis_size("tm"), lax.axis_size("space")
    first, last = tm == 0, tm == n_tm - 1
    top, bottom = sp == 0, sp == n_sp - 1
    COND, INV, W, INVK, WK = range(5)

    def load(group, hbm, lead, buf, at, count):
        out = []
        for k in range(blocks):
            cols = pl.ds(k * LANES, LANES)
            view = hbm.at[:, cols] if lead is None else hbm.at[pl.ds(lead, count), :, cols]
            dst = buf.at[at, k, pl.ds(TOP, rows), :] if lead is None else buf.at[pl.ds(at, count), k, pl.ds(TOP, rows), :]
            out.append(pltpu.make_async_copy(view, dst, load_sem.at[group, k]))
        return out

    def guess_load(group, low, count):
        return load(group, guess_hbm, low, gue, low + 1, count)

    def source_load(group, low, count):
        return load(group, source_hbm, low, src, low, count)

    loads = [
        guess_load(0, steps - 2, 2),
        load(1, cond_hbm, None, coef, COND, 1),
        source_load(2, steps - 1, 1),
        guess_load(3, steps - 4, 2),
        source_load(4, steps - 3, 2),
        guess_load(5, steps - 6, 2),
        source_load(6, steps - 5, 2),
        guess_load(7, 0, 2),
        source_load(8, 0, 3),
    ]
    starts = [load(9 + i, start_hbm, None, buf, 0, 1) for i, buf in enumerate((gue, u1, u3))]

    def start(copies):
        for c in copies:
            c.start()

    def wait(copies):
        for c in copies:
            c.wait()

    for copies in loads:
        start(copies)

    @pl.when(first)
    def _():
        for copies in starts:
            start(copies)

    barrier = pltpu.get_barrier_semaphore()

    def greet(cond, axis, index):
        @pl.when(cond)
        def _():
            pl.semaphore_signal(barrier, inc=1, device_id={axis: index}, device_id_type=MESH)

    greet(~first, "tm", tm - 1)
    greet(~last, "tm", tm + 1)
    greet(~top, "space", sp - 1)
    greet(~bottom, "space", sp + 1)
    one = jnp.int32(1)
    zero = jnp.int32(0)
    peers = (
        jnp.where(first, zero, one)
        + jnp.where(last, zero, one)
        + jnp.where(top, zero, one)
        + jnp.where(bottom, zero, one)
    )
    pl.semaphore_wait(barrier, peers)

    own = pl.ds(TOP, rows)

    def x_copy(i, buf, plane):
        return pltpu.make_async_remote_copy(
            src_ref=buf.at[plane, :, own, :],
            dst_ref=buf.at[0, :, own, :],
            send_sem=xs.at[i],
            recv_sem=xr.at[i],
            device_id={"tm": tm + 1},
            device_id_type=MESH,
        )

    x_plan = [(gue, steps), (u1, steps), (e0, half), (e1, half), (e2, half), (u3, steps)]

    def x_send(i):
        @pl.when(~last)
        def _():
            x_copy(i, *x_plan[i]).start()

    def x_wait(i):
        @pl.when(~first)
        def _():
            x_copy(i, *x_plan[i]).wait_recv()

        if i in (0, 1, 5):

            @pl.when(first)
            def _():
                wait(starts[(0, 1, 5).index(i)])

    h_plan = [
        (gue, steps - 1, 2),
        (coef, COND, 1),
        (src, steps - 1, 1),
        (gue, steps - 3, 2),
        (src, steps - 3, 2),
        (gue, steps - 5, 2),
        (src, steps - 5, 2),
        (gue, 1, 2),
        (src, 0, 3),
        (gue, 0, 1),
        (u1, 0, 1),
        (e0, 0, 1),
        (e1, 0, 1),
        (e2, 0, 1),
        (e2, half - 1, 2),
        (e2, half - 2, 1),
        (e2, 1, 1),
    ]
    OLD_GUESS, OLD_U1, OLD_E0, OLD_E1, OLD_E2, E2_LATE, E2_MID, E2_EARLY = range(9, 17)

    def down_copy(i):
        buf, plane, count = h_plan[i]
        return pltpu.make_async_remote_copy(
            src_ref=buf.at[pl.ds(plane, count), :, pl.ds(end - HALO, HALO), :],
            dst_ref=buf.at[pl.ds(plane, count), :, pl.ds(TOP - HALO, HALO), :],
            send_sem=hs.at[i, 0],
            recv_sem=hr.at[i, 0],
            device_id={"space": sp + 1},
            device_id_type=MESH,
        )

    def up_copy(i):
        buf, plane, count = h_plan[i]
        return pltpu.make_async_remote_copy(
            src_ref=buf.at[pl.ds(plane, count), :, pl.ds(TOP, HALO), :],
            dst_ref=buf.at[pl.ds(plane, count), :, pl.ds(end, HALO), :],
            send_sem=hs.at[i, 1],
            recv_sem=hr.at[i, 1],
            device_id={"space": sp - 1},
            device_id_type=MESH,
        )

    def h_send(*which):
        @pl.when(~bottom)
        def _():
            for i in which:
                down_copy(i).start()

        @pl.when(~top)
        def _():
            for i in which:
                up_copy(i).start()

    def h_wait(*which):
        @pl.when(~top)
        def _():
            for i in which:
                down_copy(i).wait_recv()

        @pl.when(~bottom)
        def _():
            for i in which:
                up_copy(i).wait_recv()

    def at(buf, n, r):
        return buf[n, :, pl.ds(r, CHUNK), :]

    def put(buf, n, r, value):
        buf[n, :, pl.ds(r, CHUNK), :] = value

    def sideways(v):
        lane = lax.broadcasted_iota(jnp.int32, v.shape, 2)
        edge = jnp.zeros((1,) + v.shape[1:], jnp.float32)
        fwd = pltpu.roll(v, 1, 2)
        bwd = pltpu.roll(v, LANES - 1, 2)
        left = jnp.where(lane == 0, jnp.concatenate([edge, fwd[:-1]], axis=0), fwd)
        right = jnp.where(lane == LANES - 1, jnp.concatenate([bwd[1:], edge], axis=0), bwd)
        return left + right

    def with_sum(buf, n, r):
        v = at(buf, n, r)
        return v, (at(buf, n, r - 1) + at(buf, n, r + 1)) + sideways(v)

    def over_rows(low, high, body):
        count = (high - low) // CHUNK

        def step(i, carry):
            body(low + i * CHUNK)
            return carry

        lax.fori_loop(0, count, step, 0, unroll=True)

    def over_planes(low, high, body):
        if high - low == 1:
            body(low)
        else:

            def step(i, carry):
                body(i)
                return carry

            lax.fori_loop(low, high, step, 0)

    wide = (TOP - HALO, end + HALO)

    def fine_smooth(frm, to, low, high):
        def first_pass(n):
            def chunk(r):
                v, s = with_sum(frm, n + 1, r)
                rest = at(src, n, r) + at(frm, n, r)
                put(tmp, n, r, damping * (at(coef, INV, r) * rest + at(coef, W, r) * s - v))

            over_rows(*wide, chunk)

        def second_pass(n):
            def chunk(r):
                v, s = with_sum(tmp, n, r)
                put(to, n + 1, r, at(frm, n + 1, r) + (v + at(coef, W, r) * s))

            over_rows(*wide, chunk)

        over_planes(low, high, first_pass)
        over_planes(low, high, second_pass)

    def restrict(m):
        def chunk(r):
            a, sa = at(u1, 2 * m + 1, r), at(u1, 2 * m + 1, r - 1) + at(u1, 2 * m + 1, r + 1)
            b, sb = at(u1, 2 * m + 2, r), at(u1, 2 * m + 2, r - 1) + at(u1, 2 * m + 2, r + 1)
            pair = a + b
            around = (sa + sb) + sideways(pair)
            total = at(src, 2 * m, r) + at(src, 2 * m + 1, r) + (at(u1, 2 * m, r) - b)
            total = total - at(coef, COND, r) * (4.0 * pair - around)
            put(rhs, m, r, at(coef, INVK, r) * total)

        over_rows(*wide, chunk)

    def coarse_first(m):
        def chunk(r):
            v, s = with_sum(rhs, m, r)
            put(e0, m + 1, r, damping * (v + at(coef, WK, r) * s))

        over_rows(*wide, chunk)

    def coarse_sweep(frm, to, m, slot):
        def first_pass(r):
            v, s = with_sum(frm, m + 1, r)
            rest = at(rhs, m, r) + at(coef, INVK, r) * at(frm, m, r)
            put(tmp, slot, r, damping * (rest + at(coef, WK, r) * s - v))

        def second_pass(r):
            v, s = with_sum(tmp, slot, r)
            put(to, m + 1, r, at(frm, m + 1, r) + (v + at(coef, WK, r) * s))

        over_rows(*wide, first_pass)
        over_rows(*((TOP, end) if to is e2 else wide), second_pass)

    def prolong_odd(m):
        over_rows(*wide, lambda r: put(u2, 2 * m + 2, r, at(u1, 2 * m + 2, r) + at(e2, m + 1, r)))

    def prolong_even(m):
        over_rows(
            *wide,
            lambda r: put(u2, 2 * m + 1, r, at(u1, 2 * m + 1, r) + 0.5 * (at(e2, m, r) + at(e2, m + 1, r))),
        )

    def last_residual(n):
        def chunk(r):
            v, s = with_sum(u3, n + 1, r)
            rest = at(src, n, r) + (at(u3, n, r) - v)
            res[n, :, pl.ds(r - TOP, CHUNK), :] = rest - at(coef, COND, r) * (4.0 * v - s)

        over_rows(TOP, end, chunk)

    def clear(low):
        zeros = jnp.zeros((blocks, HALO, LANES), jnp.float32)

        def planes(buf, a, b):
            for n in range(a, b):
                buf[n, :, pl.ds(low, HALO), :] = zeros

        planes(gue, 0, steps + 1)
        planes(src, 0, steps)
        planes(coef, COND, COND + 1)
        for buf in (u1, e0, e1):
            planes(buf, 0, 1)
        planes(e2, 0, half + 1)

    @pl.when(top)
    def _():
        clear(TOP - HALO)

    @pl.when(bottom)
    def _():
        clear(end)

    @pl.when(first)
    def _():
        for buf in (e0, e1, e2):
            buf[0, :, pl.ds(TOP, rows), :] = jnp.zeros((blocks, rows, LANES), jnp.float32)

    wait(loads[0])
    x_send(0)
    h_send(0)
    wait(loads[1])
    wait(loads[2])
    h_send(1, 2)
    wait(loads[3])
    wait(loads[4])
    h_send(3, 4)
    wait(loads[5])
    wait(loads[6])
    h_send(5, 6)
    wait(loads[7])
    wait(loads[8])
    h_send(7, 8)

    def coefficients(r):
        c = at(coef, COND, r)
        inv = 1.0 / (1.0 + 4.0 * c)
        invk = 1.0 / (1.0 + 8.0 * c)
        put(coef, INV, r, inv)
        put(coef, W, r, c * inv)
        put(coef, INVK, r, invk)
        put(coef, WK, r, (2.0 * c) * invk)

    h_wait(0, 1, 2)
    over_rows(*wide, coefficients)
    fine_smooth(gue, u1, steps - 1, steps)
    x_send(1)
    h_wait(3, 4)
    fine_smooth(gue, u1, steps - 3, steps - 1)
    restrict(half - 1)
    coarse_first(half - 1)
    x_send(2)
    h_wait(5, 6)
    fine_smooth(gue, u1, steps - 5, steps - 3)
    restrict(half - 2)
    coarse_first(half - 2)
    coarse_sweep(e0, e1, half - 1, 0)
    x_send(3)
    x_wait(0)
    h_send(OLD_GUESS)
    h_wait(7, 8)
    fine_smooth(gue, u1, 1, steps - 5)
    restrict(half - 3)
    coarse_first(half - 3)
    coarse_sweep(e0, e1, half - 2, 1)
    coarse_sweep(e1, e2, half - 1, 2)
    x_send(4)
    h_wait(OLD_GUESS)
    fine_smooth(gue, u1, 0, 1)

    x_wait(1)
    h_send(OLD_U1)
    h_wait(OLD_U1)
    restrict(0)
    coarse_first(0)
    coarse_sweep(e0, e1, 1, 3)
    coarse_sweep(e1, e2, 2, 4)
    h_send(E2_LATE)
    x_wait(2)
    h_send(OLD_E0)
    h_wait(E2_LATE)
    prolong_odd(half - 1)
    prolong_even(half - 1)
    fine_smooth(u2, u3, steps - 1, steps)
    x_send(5)
    h_wait(OLD_E0)
    coarse_sweep(e0, e1, 0, 5)
    coarse_sweep(e1, e2, 1, 6)
    h_send(E2_MID)
    prolong_odd(half - 2)
    fine_smooth(u2, u3, steps - 2, steps - 1)
    last_residual(steps - 1)
    x_wait(3)
    h_send(OLD_E1)
    h_wait(E2_MID)
    prolong_even(half - 2)
    prolong_odd(half - 3)
    fine_smooth(u2, u3, steps - 4, steps - 2)
    h_wait(OLD_E1)
    coarse_sweep(e1, e2, 0, 7)
    h_send(E2_EARLY)
    over_planes(steps - 3, steps - 1, last_residual)
    x_wait(4)
    h_send(OLD_E2)
    h_wait(E2_EARLY)
    prolong_even(1)
    prolong_odd(0)
    fine_smooth(u2, u3, 2, steps - 4)
    over_planes(3, steps - 3, last_residual)
    h_wait(OLD_E2)
    over_rows(*wide, lambda r: put(u2, 0, r, at(u1, 0, r) + at(e2, 0, r)))
    prolong_even(0)
    fine_smooth(u2, u3, 0, 2)
    over_planes(1, 3, last_residual)
    x_wait(5)
    last_residual(0)

    @pl.when(~last)
    def _():
        for i in range(len(x_plan)):
            x_copy(i, *x_plan[i]).wait_send()

    @pl.when(~bottom)
    def _():
        for i in range(len(h_plan)):
            down_copy(i).wait_send()

    @pl.when(~top)
    def _():
        for i in range(len(h_plan)):
            up_copy(i).wait_send()


def store_kernel(steps, rows, blocks, u3, res, field_out, res_out, sem):
    copies = []
    for k in range(blocks):
        cols = pl.ds(k * LANES, LANES)
        copies.append(
            pltpu.make_async_copy(
                u3.at[pl.ds(1, steps), k, pl.ds(TOP, rows), :], field_out.at[:, :, cols], sem.at[0, k]
            )
        )
        copies.append(pltpu.make_async_copy(res.at[:, k, :, :], res_out.at[:, :, cols], sem.at[1, k]))
    for c in copies:
        c.start()
    for c in copies:
        c.wait()


def shards(source, guess, start_state, conduct):
    steps, rows, cols = source.shape
    blocks = cols // LANES
    half = steps // 2
    tall = rows + 2 * TOP
    f32 = jnp.float32
    hbm = pl.BlockSpec(memory_space=pltpu.HBM)
    vmem = pl.BlockSpec(memory_space=pltpu.VMEM)

    def planes(n):
        return pltpu.VMEM((n, blocks, tall, LANES), f32)

    u3, res = pl.pallas_call(
        functools.partial(cycle_kernel, steps, rows, blocks),
        out_shape=(
            jax.ShapeDtypeStruct((steps + 1, blocks, tall, LANES), f32),
            jax.ShapeDtypeStruct((steps, blocks, rows, LANES), f32),
        ),
        in_specs=[hbm] * 4,
        out_specs=(vmem, vmem),
        scratch_shapes=[
            planes(steps),
            planes(steps + 1),
            planes(steps + 1),
            planes(steps + 1),
            planes(half + 1),
            planes(half + 1),
            planes(half + 1),
            planes(half),
            planes(steps),
            planes(5),
            pltpu.SemaphoreType.DMA((12, blocks)),
            pltpu.SemaphoreType.DMA((6,)),
            pltpu.SemaphoreType.DMA((6,)),
            pltpu.SemaphoreType.DMA((17, 2)),
            pltpu.SemaphoreType.DMA((17, 2)),
        ],
        compiler_params=pltpu.CompilerParams(
            collective_id=0, has_side_effects=True, vmem_limit_bytes=44 * 1024 * 1024
        ),
        name="cycle",
    )(*(pltpu.with_memory_space_constraint(a, pltpu.HBM) for a in (source, guess, start_state, conduct)))
    return pl.pallas_call(
        functools.partial(store_kernel, steps, rows, blocks),
        out_shape=(jax.ShapeDtypeStruct(source.shape, f32), jax.ShapeDtypeStruct(source.shape, f32)),
        in_specs=[vmem, vmem],
        out_specs=(hbm, hbm),
        scratch_shapes=[pltpu.SemaphoreType.DMA((2, blocks))],
        compiler_params=pltpu.CompilerParams(vmem_limit_bytes=16 * 1024 * 1024),
        name="store",
    )(u3, res)


def solution(mesh):
    return jax.shard_map(
        shards,
        mesh=mesh,
        in_specs=(
            P("tm", "space", None),
            P("tm", "space", None),
            P("space", None),
            P("space", None),
        ),
        out_specs=(P("tm", "space", None), P("tm", "space", None)),
        check_vma=False,
    )
```

```python
import functools

import jax
import jax.numpy as jnp
from jax import lax
from jax.experimental import pallas as pl
from jax.experimental.pallas import tpu as pltpu
from jax.sharding import PartitionSpec as P

damping = 0.8
MESH = pl.DeviceIdType.MESH
LANES = 128
HALO = 12
TOP = 16
CHUNK = 8
EDGE = 24


def cycle_kernel(
    steps,
    rows,
    blocks,
    source_hbm,
    guess_hbm,
    start_hbm,
    cond_hbm,
    u3,
    res,
    src,
    gue,
    u1,
    u2,
    e0,
    e1,
    e2,
    rhs,
    tmp,
    coef,
    sums,
    relay,
    load_sem,
    xs,
    xr,
    ls,
    lr,
    fs,
    hs,
    hr,
):
    half = steps // 2
    end = TOP + rows
    tm, sp = lax.axis_index("tm"), lax.axis_index("space")
    n_tm, n_sp = lax.axis_size("tm"), lax.axis_size("space")
    first, last = tm == 0, tm == n_tm - 1
    top, bottom = sp == 0, sp == n_sp - 1
    COND, INV, W, INVK, WK = range(5)

    def load(group, hbm, lead, buf, at, count):
        out = []
        for k in range(blocks):
            cols = pl.ds(k * LANES, LANES)
            view = hbm.at[:, cols] if lead is None else hbm.at[pl.ds(lead, count), :, cols]
            dst = buf.at[at, k, pl.ds(TOP, rows), :] if lead is None else buf.at[pl.ds(at, count), k, pl.ds(TOP, rows), :]
            out.append(pltpu.make_async_copy(view, dst, load_sem.at[group, k]))
        return out

    def guess_load(group, low, count):
        return load(group, guess_hbm, low, gue, low + 1, count)

    def source_load(group, low, count):
        return load(group, source_hbm, low, src, low, count)

    loads = [
        guess_load(0, steps - 2, 2),
        load(1, cond_hbm, None, coef, COND, 1),
        source_load(2, steps - 1, 1),
        guess_load(3, steps - 4, 2),
        source_load(4, steps - 3, 2),
        guess_load(5, steps - 6, 2),
        source_load(6, steps - 5, 2),
        guess_load(7, 0, 2),
        source_load(8, 0, 3),
    ]
    starts = [load(9 + i, start_hbm, None, buf, 0, 1) for i, buf in enumerate((gue, u3))]

    def start(copies):
        for c in copies:
            c.start()

    def wait(copies):
        for c in copies:
            c.wait()

    for copies in loads:
        start(copies)

    @pl.when(first)
    def _():
        for copies in starts:
            start(copies)

    barrier = pltpu.get_barrier_semaphore()

    def greet(cond, axis, index):
        @pl.when(cond)
        def _():
            pl.semaphore_signal(barrier, inc=1, device_id={axis: index}, device_id_type=MESH)

    for other in range(n_tm):
        greet(tm != other, "tm", other)
    greet(~top, "space", sp - 1)
    greet(~bottom, "space", sp + 1)
    one = jnp.int32(1)
    zero = jnp.int32(0)
    pl.semaphore_wait(barrier, (n_tm - 1) + jnp.where(top, zero, one) + jnp.where(bottom, zero, one))

    x_plan = [(gue, steps), (sums, 1), (e0, half), (e1, half), (e2, half), (u3, steps)]
    pieces = [(TOP, EDGE), (end - EDGE, EDGE), (TOP + EDGE, rows - 2 * EDGE)]
    MIDDLE = 2
    relayed = {1: 0, 2: 1, 3: 2, 5: 3}
    ways = {0: (3, 0), 1: (3, 1), 2: (1, 0)}
    relays = {3: ((0, 1), (1, 2)), 1: ((0, 3),)}

    def x_copy(i, piece):
        buf, plane = x_plan[i]
        part = pl.ds(*pieces[piece])
        return pltpu.make_async_remote_copy(
            src_ref=buf.at[plane, :, part, :],
            dst_ref=buf.at[0, :, part, :],
            send_sem=xs.at[i, piece],
            recv_sem=xr.at[i, piece],
            device_id={"tm": tm + 1},
            device_id_type=MESH,
        )

    def to_relay(i, device, slot):
        buf, plane = x_plan[i]
        return pltpu.make_async_remote_copy(
            src_ref=buf.at[plane, :, pl.ds(*pieces[MIDDLE]), :],
            dst_ref=relay.at[slot, relayed[i]],
            send_sem=ls.at[relayed[i]],
            recv_sem=lr.at[slot, relayed[i]],
            device_id={"tm": device},
            device_id_type=MESH,
        )

    def from_relay(i, slot, device):
        return pltpu.make_async_remote_copy(
            src_ref=relay.at[slot, relayed[i]],
            dst_ref=x_plan[i][0].at[0, :, pl.ds(*pieces[MIDDLE]), :],
            send_sem=fs.at[slot, relayed[i]],
            recv_sem=xr.at[i, MIDDLE],
            device_id={"tm": device},
            device_id_type=MESH,
        )

    def direct(i):
        return (0, 1) if i in relayed else (0, 1, 2)

    def x_send(i):
        if i in relayed:
            for sender, way in ways.items():

                @pl.when(tm == sender)
                def _():
                    to_relay(i, *way).start()

        @pl.when(~last)
        def _():
            for piece in direct(i):
                x_copy(i, piece).start()

    def x_relay(i):
        for device, jobs in relays.items():

            @pl.when(tm == device)
            def _():
                for slot, final in jobs:
                    to_relay(i, device, slot).wait_recv()
                    from_relay(i, slot, final).start()

    def x_edges(i):
        @pl.when(~first)
        def _():
            for piece in (0, 1):
                x_copy(i, piece).wait_recv()

        if i in (0, 5):

            @pl.when(first)
            def _():
                wait(starts[(0, 5).index(i)])

    def x_middle(i):
        @pl.when(~first)
        def _():
            x_copy(i, MIDDLE).wait_recv()

    h_plan = [
        (gue, steps - 1, 2, 11),
        (coef, COND, 1, 10),
        (src, steps - 1, 1, 10),
        (gue, steps - 3, 2, 11),
        (src, steps - 3, 2, 10),
        (gue, steps - 5, 2, 11),
        (src, steps - 5, 2, 10),
        (gue, 1, 2, 11),
        (src, 0, 3, 10),
        (gue, 0, 1, 10),
        (sums, 0, 1, 9),
        (e0, 0, 1, 6),
        (e1, 0, 1, 4),
        (e2, 0, 1, 3),
    ]
    OLD_GUESS, OLD_SUM, OLD_E0, OLD_E1, OLD_E2 = range(9, 14)

    def down_copy(i):
        buf, plane, count, width = h_plan[i]
        return pltpu.make_async_remote_copy(
            src_ref=buf.at[pl.ds(plane, count), :, pl.ds(end - width, width), :],
            dst_ref=buf.at[pl.ds(plane, count), :, pl.ds(TOP - width, width), :],
            send_sem=hs.at[i, 0],
            recv_sem=hr.at[i, 0],
            device_id={"space": sp + 1},
            device_id_type=MESH,
        )

    def up_copy(i):
        buf, plane, count, width = h_plan[i]
        return pltpu.make_async_remote_copy(
            src_ref=buf.at[pl.ds(plane, count), :, pl.ds(TOP, width), :],
            dst_ref=buf.at[pl.ds(plane, count), :, pl.ds(end, width), :],
            send_sem=hs.at[i, 1],
            recv_sem=hr.at[i, 1],
            device_id={"space": sp - 1},
            device_id_type=MESH,
        )

    def h_send(*which):
        @pl.when(~bottom)
        def _():
            for i in which:
                down_copy(i).start()

        @pl.when(~top)
        def _():
            for i in which:
                up_copy(i).start()

    def h_wait(*which):
        @pl.when(~top)
        def _():
            for i in which:
                down_copy(i).wait_recv()

        @pl.when(~bottom)
        def _():
            for i in which:
                up_copy(i).wait_recv()

    def at(buf, n, r):
        return buf[n, :, pl.ds(r, CHUNK), :]

    def put(buf, n, r, value):
        buf[n, :, pl.ds(r, CHUNK), :] = value

    def sideways(v):
        lane = lax.broadcasted_iota(jnp.int32, v.shape, 2)
        edge = jnp.zeros((1,) + v.shape[1:], jnp.float32)
        fwd = pltpu.roll(v, 1, 2)
        bwd = pltpu.roll(v, LANES - 1, 2)
        left = jnp.where(lane == 0, jnp.concatenate([edge, fwd[:-1]], axis=0), fwd)
        right = jnp.where(lane == LANES - 1, jnp.concatenate([bwd[1:], edge], axis=0), bwd)
        return left + right

    def with_sum(buf, n, r):
        v = at(buf, n, r)
        return v, (at(buf, n, r - 1) + at(buf, n, r + 1)) + sideways(v)

    def over_rows(low, high, body):
        count = (high - low) // CHUNK

        def step(i, carry):
            body(low + i * CHUNK)
            return carry

        lax.fori_loop(0, count, step, 0, unroll=True)

    def over_planes(low, high, body):
        if high - low == 1:
            body(low)
        else:

            def step(i, carry):
                body(i)
                return carry

            lax.fori_loop(low, high, step, 0)

    def grown(extra):
        return (TOP - extra, end + extra)

    fine_rows, coarse_rows, late_rows = grown(12), grown(8), grown(4)

    def fine_smooth(frm, to, low, high, where):
        def first_pass(n):
            def chunk(r):
                v, s = with_sum(frm, n + 1, r)
                rest = at(src, n, r) + at(frm, n, r)
                put(tmp, n, r, damping * (at(coef, INV, r) * rest + at(coef, W, r) * s - v))

            over_rows(*where, chunk)

        def second_pass(n):
            def chunk(r):
                v, s = with_sum(tmp, n, r)
                put(to, n + 1, r, at(frm, n + 1, r) + (v + at(coef, W, r) * s))

            over_rows(*where, chunk)

        over_planes(low, high, first_pass)
        over_planes(low, high, second_pass)

    def smooth_before():
        def first_pass(r):
            v, s = with_sum(gue, 0, r)
            put(tmp, 0, r, damping * (at(coef, INV, r) * at(sums, 0, r) + at(coef, W, r) * s - v))

        def second_pass(r):
            v, s = with_sum(tmp, 0, r)
            put(u1, 0, r, at(gue, 0, r) + (v + at(coef, W, r) * s))

        @pl.when(first)
        def _():
            over_rows(*fine_rows, lambda r: put(u1, 0, r, at(gue, 0, r)))

        @pl.when(~first)
        def _():
            over_rows(*fine_rows, first_pass)
            over_rows(*fine_rows, second_pass)

    def restrict(m):
        def chunk(r):
            a, sa = at(u1, 2 * m + 1, r), at(u1, 2 * m + 1, r - 1) + at(u1, 2 * m + 1, r + 1)
            b, sb = at(u1, 2 * m + 2, r), at(u1, 2 * m + 2, r - 1) + at(u1, 2 * m + 2, r + 1)
            pair = a + b
            around = (sa + sb) + sideways(pair)
            total = at(src, 2 * m, r) + at(src, 2 * m + 1, r) + (at(u1, 2 * m, r) - b)
            total = total - at(coef, COND, r) * (4.0 * pair - around)
            put(rhs, m, r, at(coef, INVK, r) * total)

        over_rows(*coarse_rows, chunk)

    def coarse_first(m):
        def chunk(r):
            v, s = with_sum(rhs, m, r)
            put(e0, m + 1, r, damping * (v + at(coef, WK, r) * s))

        over_rows(*coarse_rows, chunk)

    def coarse_sweep(frm, to, m, slot):
        def first_pass(r):
            v, s = with_sum(frm, m + 1, r)
            rest = at(rhs, m, r) + at(coef, INVK, r) * at(frm, m, r)
            put(tmp, slot, r, damping * (rest + at(coef, WK, r) * s - v))

        def second_pass(r):
            v, s = with_sum(tmp, slot, r)
            put(to, m + 1, r, at(frm, m + 1, r) + (v + at(coef, WK, r) * s))

        where = late_rows if to is e2 else coarse_rows
        over_rows(*where, first_pass)
        over_rows(*where, second_pass)

    def prolong_odd(m):
        over_rows(*late_rows, lambda r: put(u2, 2 * m + 2, r, at(u1, 2 * m + 2, r) + at(e2, m + 1, r)))

    def prolong_even(m):
        over_rows(
            *late_rows,
            lambda r: put(u2, 2 * m + 1, r, at(u1, 2 * m + 1, r) + 0.5 * (at(e2, m, r) + at(e2, m + 1, r))),
        )

    def last_residual(n):
        def chunk(r):
            v, s = with_sum(u3, n + 1, r)
            rest = at(src, n, r) + (at(u3, n, r) - v)
            res[n, :, pl.ds(r - TOP, CHUNK), :] = rest - at(coef, COND, r) * (4.0 * v - s)

        over_rows(TOP, end, chunk)

    def clear(low):
        zeros = jnp.zeros((blocks, HALO, LANES), jnp.float32)

        def planes(buf, a, b):
            for n in range(a, b):
                buf[n, :, pl.ds(low, HALO), :] = zeros

        planes(gue, 0, steps + 1)
        planes(src, 0, steps)
        planes(coef, COND, COND + 1)
        for buf in (sums, e0, e1, e2):
            planes(buf, 0, 1)

    @pl.when(top)
    def _():
        clear(TOP - HALO)

    @pl.when(bottom)
    def _():
        clear(end)

    @pl.when(first)
    def _():
        for buf in (sums, e0, e1, e2):
            buf[0, :, pl.ds(TOP, rows), :] = jnp.zeros((blocks, rows, LANES), jnp.float32)

    wait(loads[0])
    x_send(0)
    h_send(0)
    wait(loads[1])
    wait(loads[2])
    over_rows(TOP, end, lambda r: put(sums, 1, r, at(src, steps - 1, r) + at(gue, steps - 1, r)))
    h_send(1, 2)
    x_send(1)
    wait(loads[3])
    wait(loads[4])
    h_send(3, 4)
    wait(loads[5])
    wait(loads[6])
    h_send(5, 6)
    wait(loads[7])
    wait(loads[8])
    h_send(7, 8)

    def coefficients(r):
        c = at(coef, COND, r)
        inv = 1.0 / (1.0 + 4.0 * c)
        invk = 1.0 / (1.0 + 8.0 * c)
        put(coef, INV, r, inv)
        put(coef, W, r, c * inv)
        put(coef, INVK, r, invk)
        put(coef, WK, r, (2.0 * c) * invk)

    h_wait(0, 1, 2)
    over_rows(*fine_rows, coefficients)
    fine_smooth(gue, u1, steps - 1, steps, fine_rows)
    h_wait(3, 4)
    fine_smooth(gue, u1, steps - 3, steps - 1, fine_rows)
    restrict(half - 1)
    coarse_first(half - 1)
    x_send(2)
    x_edges(0)
    h_send(OLD_GUESS)
    x_relay(1)
    h_wait(5, 6)
    fine_smooth(gue, u1, steps - 5, steps - 3, fine_rows)
    restrict(half - 2)
    coarse_first(half - 2)
    coarse_sweep(e0, e1, half - 1, 0)
    x_send(3)
    x_edges(1)
    h_send(OLD_SUM)
    h_wait(7, 8)
    fine_smooth(gue, u1, 1, steps - 5, fine_rows)
    restrict(half - 3)
    coarse_first(half - 3)
    coarse_sweep(e0, e1, half - 2, 1)
    coarse_sweep(e1, e2, half - 1, 2)
    x_send(4)
    h_wait(OLD_GUESS)
    x_middle(0)
    fine_smooth(gue, u1, 0, 1, fine_rows)

    h_wait(OLD_SUM)
    x_middle(1)
    smooth_before()
    restrict(0)
    coarse_first(0)
    x_edges(2)
    h_send(OLD_E0)
    coarse_sweep(e0, e1, 1, 3)
    coarse_sweep(e1, e2, 2, 4)
    x_relay(2)
    prolong_odd(half - 1)
    prolong_even(half - 1)
    fine_smooth(u2, u3, steps - 1, steps, late_rows)
    x_send(5)
    prolong_odd(half - 2)
    fine_smooth(u2, u3, steps - 2, steps - 1, late_rows)
    last_residual(steps - 1)
    x_relay(3)
    x_edges(3)
    h_send(OLD_E1)
    h_wait(OLD_E0)
    x_middle(2)
    coarse_sweep(e0, e1, 0, 5)
    coarse_sweep(e1, e2, 1, 6)
    prolong_even(half - 2)
    prolong_odd(half - 3)
    fine_smooth(u2, u3, steps - 4, steps - 2, late_rows)
    h_wait(OLD_E1)
    x_middle(3)
    coarse_sweep(e1, e2, 0, 7)
    x_edges(4)
    h_send(OLD_E2)
    x_relay(5)
    over_planes(steps - 3, steps - 1, last_residual)
    prolong_even(1)
    prolong_odd(0)
    fine_smooth(u2, u3, 2, steps - 4, late_rows)
    over_planes(3, steps - 3, last_residual)
    h_wait(OLD_E2)
    x_middle(4)
    over_rows(*late_rows, lambda r: put(u2, 0, r, at(u1, 0, r) + at(e2, 0, r)))
    prolong_even(0)
    fine_smooth(u2, u3, 0, 2, late_rows)
    over_planes(1, 3, last_residual)
    x_edges(5)
    x_middle(5)
    last_residual(0)

    @pl.when(~last)
    def _():
        for i in range(len(x_plan)):
            for piece in direct(i):
                x_copy(i, piece).wait_send()
        for i in relayed:
            to_relay(i, 0, 0).wait_send()

    for device, jobs in relays.items():

        @pl.when(tm == device)
        def _():
            for i in relayed:
                for slot, final in jobs:
                    from_relay(i, slot, final).wait_send()

    @pl.when(~bottom)
    def _():
        for i in range(len(h_plan)):
            down_copy(i).wait_send()

    @pl.when(~top)
    def _():
        for i in range(len(h_plan)):
            up_copy(i).wait_send()


def store_kernel(steps, rows, blocks, u3, res, field_out, res_out, sem):
    copies = []
    for k in range(blocks):
        cols = pl.ds(k * LANES, LANES)
        copies.append(
            pltpu.make_async_copy(
                u3.at[pl.ds(1, steps), k, pl.ds(TOP, rows), :], field_out.at[:, :, cols], sem.at[0, k]
            )
        )
        copies.append(pltpu.make_async_copy(res.at[:, k, :, :], res_out.at[:, :, cols], sem.at[1, k]))
    for c in copies:
        c.start()
    for c in copies:
        c.wait()


def shards(source, guess, start_state, conduct):
    steps, rows, cols = source.shape
    blocks = cols // LANES
    half = steps // 2
    tall = rows + 2 * TOP
    f32 = jnp.float32
    hbm = pl.BlockSpec(memory_space=pltpu.HBM)
    vmem = pl.BlockSpec(memory_space=pltpu.VMEM)

    def planes(n):
        return pltpu.VMEM((n, blocks, tall, LANES), f32)

    u3, res = pl.pallas_call(
        functools.partial(cycle_kernel, steps, rows, blocks),
        out_shape=(
            jax.ShapeDtypeStruct((steps + 1, blocks, tall, LANES), f32),
            jax.ShapeDtypeStruct((steps, blocks, rows, LANES), f32),
        ),
        in_specs=[hbm] * 4,
        out_specs=(vmem, vmem),
        scratch_shapes=[
            planes(steps),
            planes(steps + 1),
            planes(steps + 1),
            planes(steps + 1),
            planes(half + 1),
            planes(half + 1),
            planes(half + 1),
            planes(half),
            planes(steps),
            planes(5),
            planes(2),
            pltpu.VMEM((2, 4, blocks, rows - 2 * EDGE, LANES), f32),
            pltpu.SemaphoreType.DMA((11, blocks)),
            pltpu.SemaphoreType.DMA((6, 3)),
            pltpu.SemaphoreType.DMA((6, 3)),
            pltpu.SemaphoreType.DMA((4,)),
            pltpu.SemaphoreType.DMA((2, 4)),
            pltpu.SemaphoreType.DMA((2, 4)),
            pltpu.SemaphoreType.DMA((14, 2)),
            pltpu.SemaphoreType.DMA((14, 2)),
        ],
        compiler_params=pltpu.CompilerParams(
            collective_id=0, has_side_effects=True, vmem_limit_bytes=44 * 1024 * 1024
        ),
        name="cycle",
    )(*(pltpu.with_memory_space_constraint(a, pltpu.HBM) for a in (source, guess, start_state, conduct)))
    return pl.pallas_call(
        functools.partial(store_kernel, steps, rows, blocks),
        out_shape=(jax.ShapeDtypeStruct(source.shape, f32), jax.ShapeDtypeStruct(source.shape, f32)),
        in_specs=[vmem, vmem],
        out_specs=(hbm, hbm),
        scratch_shapes=[pltpu.SemaphoreType.DMA((2, blocks))],
        compiler_params=pltpu.CompilerParams(vmem_limit_bytes=16 * 1024 * 1024),
        name="store",
    )(u3, res)


def solution(mesh):
    return jax.shard_map(
        shards,
        mesh=mesh,
        in_specs=(
            P("tm", "space", None),
            P("tm", "space", None),
            P("space", None),
            P("space", None),
        ),
        out_specs=(P("tm", "space", None), P("tm", "space", None)),
        check_vma=False,
    )
```

```python
import functools

import jax
import jax.numpy as jnp
from jax import lax
from jax.experimental import pallas as pl
from jax.experimental.pallas import tpu as pltpu
from jax.sharding import PartitionSpec as P

damping = 0.8
MESH = pl.DeviceIdType.MESH
LANES = 128
HALO = 12
TOP = 16
CHUNK = 8
EDGE = (12, 12, 8, 8, 8, 8)
AROUND = (8, 16, 8, 12, 12, 16)


def cycle_kernel(
    steps,
    rows,
    blocks,
    source_hbm,
    guess_hbm,
    start_hbm,
    cond_hbm,
    u3,
    res,
    src,
    gue,
    u1,
    u2,
    e0,
    e1,
    e2,
    rhs,
    tmp,
    coef,
    sums,
    relay,
    load_sem,
    xs,
    xr,
    lr,
    fs,
    hs,
    hr,
):
    half = steps // 2
    end = TOP + rows
    tm, sp = lax.axis_index("tm"), lax.axis_index("space")
    n_tm, n_sp = lax.axis_size("tm"), lax.axis_size("space")
    first, last = tm == 0, tm == n_tm - 1
    top, bottom = sp == 0, sp == n_sp - 1
    COND, INV, W, INVK, WK = range(5)

    def rows_wait(sem, count):
        planes = next(n for n in range(1, count + 1) if count % n == 0 and count // n <= end)
        there = gue.at[pl.ds(0, planes), :, pl.ds(0, count // planes), :]
        pltpu.make_async_copy(there, there, sem).wait()

    def load(group, hbm, lead, buf, at, count):
        out = []
        for k in range(blocks):
            cols = pl.ds(k * LANES, LANES)
            view = hbm.at[:, cols] if lead is None else hbm.at[pl.ds(lead, count), :, cols]
            dst = buf.at[at, k, pl.ds(TOP, rows), :] if lead is None else buf.at[pl.ds(at, count), k, pl.ds(TOP, rows), :]
            out.append(pltpu.make_async_copy(view, dst, load_sem.at[group]))
        return out

    def guess_load(group, low, count):
        return load(group, guess_hbm, low, gue, low + 1, count)

    def source_load(group, low, count):
        return load(group, source_hbm, low, src, low, count)

    def load_wait(group):
        rows_wait(load_sem.at[group], rows * (2, 2, 4, 4, 5, 1, 1)[group])

    for copies in (
        guess_load(0, steps - 2, 2),
        load(1, cond_hbm, None, coef, COND, 1),
        source_load(1, steps - 1, 1),
        guess_load(2, steps - 4, 2),
        source_load(2, steps - 3, 2),
        guess_load(3, steps - 6, 2),
        source_load(3, steps - 5, 2),
        guess_load(4, 0, 2),
        source_load(4, 0, 3),
    ):
        for c in copies:
            c.start()

    @pl.when(first)
    def _():
        for i, buf in enumerate((gue, u3)):
            for c in load(5 + i, start_hbm, None, buf, 0, 1):
                c.start()

    barrier = pltpu.get_barrier_semaphore()

    def greet(cond, axis, index):
        @pl.when(cond)
        def _():
            pl.semaphore_signal(barrier, inc=1, device_id={axis: index}, device_id_type=MESH)

    for other in range(n_tm):
        greet((tm != other) & (tm + other != 2), "tm", other)
    greet(~top, "space", sp - 1)
    greet(~bottom, "space", sp + 1)
    one = jnp.int32(1)
    zero = jnp.int32(0)
    peers = jnp.where((tm == 1) | (tm == 3), one * 3, one * 2)
    pl.semaphore_wait(barrier, peers + jnp.where(top, zero, one) + jnp.where(bottom, zero, one))

    x_plan = [(gue, steps), (sums, 1), (e0, half), (e1, half), (e2, half), (u3, steps)]
    ways = {0: (3, 0), 1: (3, 1), 2: (1, 0)}
    relays = {3: ((0, 1), (1, 2)), 1: ((0, 3),)}
    FIRST_ROWS, LAST_ROWS, INNER, AROUND_ROWS = range(4)

    def part(i, piece):
        edge, inner = EDGE[i], rows - 2 * EDGE[i] - AROUND[i]
        return pl.ds(
            *((TOP, edge), (end - edge, edge), (TOP + edge, inner), (TOP + edge + inner, AROUND[i]))[piece]
        )

    def x_copy(i, piece):
        buf, plane = x_plan[i]
        return pltpu.make_async_remote_copy(
            src_ref=buf.at[plane, :, part(i, piece), :],
            dst_ref=buf.at[0, :, part(i, piece), :],
            send_sem=xs,
            recv_sem=xr.at[i, piece // 2],
            device_id={"tm": tm + 1},
            device_id_type=MESH,
        )

    def to_relay(i, device, slot):
        buf, plane = x_plan[i]
        return pltpu.make_async_remote_copy(
            src_ref=buf.at[plane, :, part(i, AROUND_ROWS), :],
            dst_ref=relay.at[slot, i, :, pl.ds(0, AROUND[i]), :],
            send_sem=xs,
            recv_sem=lr.at[slot, i],
            device_id={"tm": device},
            device_id_type=MESH,
        )

    def from_relay(i, slot, device):
        return pltpu.make_async_remote_copy(
            src_ref=relay.at[slot, i, :, pl.ds(0, AROUND[i]), :],
            dst_ref=x_plan[i][0].at[0, :, part(i, AROUND_ROWS), :],
            send_sem=fs.at[slot],
            recv_sem=xr.at[i, 1],
            device_id={"tm": device},
            device_id_type=MESH,
        )

    def x_send_edges(i):
        @pl.when(~last)
        def _():
            x_copy(i, FIRST_ROWS).start()
            x_copy(i, LAST_ROWS).start()

        for sender, way in ways.items():

            @pl.when(tm == sender)
            def _():
                to_relay(i, *way).start()

    def x_send_inner(*which):
        @pl.when(~last)
        def _():
            for i in which:
                x_copy(i, INNER).start()

    def x_send(i):
        x_send_edges(i)
        x_send_inner(i)

    def x_relay(i):
        for device, jobs in relays.items():

            @pl.when(tm == device)
            def _():
                for slot, final in jobs:
                    to_relay(i, device, slot).wait_recv()
                    from_relay(i, slot, final).start()

    def x_edges(i):
        @pl.when(~first)
        def _():
            rows_wait(xr.at[i, 0], 2 * EDGE[i])

        if i in (0, 5):

            @pl.when(first)
            def _():
                load_wait(5 if i == 0 else 6)

    def x_inner(i):
        @pl.when(~first)
        def _():
            rows_wait(xr.at[i, 1], rows - 2 * EDGE[i])

    h_plan = [
        ((gue, steps - 1, 2, 11), (coef, COND, 1, 10), (src, steps - 1, 1, 10)),
        ((gue, steps - 3, 2, 11), (src, steps - 3, 2, 10)),
        ((gue, steps - 5, 2, 11), (src, steps - 5, 2, 10)),
        ((gue, 1, 2, 11), (src, 0, 3, 10)),
        ((gue, 0, 1, 10),),
        ((sums, 0, 1, 9),),
        ((e0, 0, 1, 6),),
        ((e1, 0, 1, 4),),
        ((e2, 0, 1, 3),),
    ]
    OLD_GUESS, OLD_SUM, OLD_E0, OLD_E1, OLD_E2 = range(4, 9)

    def down_copy(i, buf, plane, count, width):
        return pltpu.make_async_remote_copy(
            src_ref=buf.at[pl.ds(plane, count), :, pl.ds(end - width, width), :],
            dst_ref=buf.at[pl.ds(plane, count), :, pl.ds(TOP - width, width), :],
            send_sem=hs.at[0],
            recv_sem=hr.at[i, 0],
            device_id={"space": sp + 1},
            device_id_type=MESH,
        )

    def up_copy(i, buf, plane, count, width):
        return pltpu.make_async_remote_copy(
            src_ref=buf.at[pl.ds(plane, count), :, pl.ds(TOP, width), :],
            dst_ref=buf.at[pl.ds(plane, count), :, pl.ds(end, width), :],
            send_sem=hs.at[1],
            recv_sem=hr.at[i, 1],
            device_id={"space": sp - 1},
            device_id_type=MESH,
        )

    def h_send(i, low=0, high=9):
        @pl.when(~bottom)
        def _():
            for item in h_plan[i][low:high]:
                down_copy(i, *item).start()

        @pl.when(~top)
        def _():
            for item in h_plan[i][low:high]:
                up_copy(i, *item).start()

    def h_rows(group):
        return sum(count * width for _, _, count, width in group)

    def h_wait(i):
        @pl.when(~top)
        def _():
            rows_wait(hr.at[i, 0], h_rows(h_plan[i]))

        @pl.when(~bottom)
        def _():
            rows_wait(hr.at[i, 1], h_rows(h_plan[i]))

    def at(buf, n, r):
        return buf[n, :, pl.ds(r, CHUNK), :]

    def put(buf, n, r, value):
        buf[n, :, pl.ds(r, CHUNK), :] = value

    def sideways(v):
        lane = lax.broadcasted_iota(jnp.int32, v.shape, 2)
        edge = jnp.zeros((1,) + v.shape[1:], jnp.float32)
        fwd = pltpu.roll(v, 1, 2)
        bwd = pltpu.roll(v, LANES - 1, 2)
        left = jnp.where(lane == 0, jnp.concatenate([edge, fwd[:-1]], axis=0), fwd)
        right = jnp.where(lane == LANES - 1, jnp.concatenate([bwd[1:], edge], axis=0), bwd)
        return left + right

    def with_sum(buf, n, r):
        v = at(buf, n, r)
        return v, (at(buf, n, r - 1) + at(buf, n, r + 1)) + sideways(v)

    def over_rows(low, high, body):
        count = (high - low) // CHUNK

        def step(i, carry):
            body(low + i * CHUNK)
            return carry

        lax.fori_loop(0, count, step, 0, unroll=True)

    def over_planes(low, high, body):
        if high - low == 1:
            body(low)
        else:

            def step(i, carry):
                body(i)
                return carry

            lax.fori_loop(low, high, step, 0)

    def grown(extra):
        return (TOP - extra, end + extra)

    fine_rows, coarse_rows, late_rows = grown(12), grown(8), grown(4)

    def fine_smooth(frm, to, low, high, where):
        def first_pass(n):
            def chunk(r):
                v, s = with_sum(frm, n + 1, r)
                rest = at(src, n, r) + at(frm, n, r)
                put(tmp, n, r, damping * (at(coef, INV, r) * rest + at(coef, W, r) * s - v))

            over_rows(*where, chunk)

        def second_pass(n):
            def chunk(r):
                v, s = with_sum(tmp, n, r)
                put(to, n + 1, r, at(frm, n + 1, r) + (v + at(coef, W, r) * s))

            over_rows(*where, chunk)

        over_planes(low, high, first_pass)
        over_planes(low, high, second_pass)

    def smooth_before():
        def first_pass(r):
            v, s = with_sum(gue, 0, r)
            put(tmp, 0, r, damping * (at(coef, INV, r) * at(sums, 0, r) + at(coef, W, r) * s - v))

        def second_pass(r):
            v, s = with_sum(tmp, 0, r)
            put(u1, 0, r, at(gue, 0, r) + (v + at(coef, W, r) * s))

        @pl.when(first)
        def _():
            over_rows(*fine_rows, lambda r: put(u1, 0, r, at(gue, 0, r)))

        @pl.when(~first)
        def _():
            over_rows(*fine_rows, first_pass)
            over_rows(*fine_rows, second_pass)

    def restrict(m):
        def chunk(r):
            a, sa = at(u1, 2 * m + 1, r), at(u1, 2 * m + 1, r - 1) + at(u1, 2 * m + 1, r + 1)
            b, sb = at(u1, 2 * m + 2, r), at(u1, 2 * m + 2, r - 1) + at(u1, 2 * m + 2, r + 1)
            pair = a + b
            around = (sa + sb) + sideways(pair)
            total = at(src, 2 * m, r) + at(src, 2 * m + 1, r) + (at(u1, 2 * m, r) - b)
            total = total - at(coef, COND, r) * (4.0 * pair - around)
            put(rhs, m, r, at(coef, INVK, r) * total)

        over_rows(*coarse_rows, chunk)

    def coarse_first(m):
        def chunk(r):
            v, s = with_sum(rhs, m, r)
            put(e0, m + 1, r, damping * (v + at(coef, WK, r) * s))

        over_rows(*coarse_rows, chunk)

    def coarse_sweep(frm, to, m, slot):
        def first_pass(r):
            v, s = with_sum(frm, m + 1, r)
            rest = at(rhs, m, r) + at(coef, INVK, r) * at(frm, m, r)
            put(tmp, slot, r, damping * (rest + at(coef, WK, r) * s - v))

        def second_pass(r):
            v, s = with_sum(tmp, slot, r)
            put(to, m + 1, r, at(frm, m + 1, r) + (v + at(coef, WK, r) * s))

        where = late_rows if to is e2 else coarse_rows
        over_rows(*where, first_pass)
        over_rows(*where, second_pass)

    def prolong_odd(m):
        over_rows(*late_rows, lambda r: put(u2, 2 * m + 2, r, at(u1, 2 * m + 2, r) + at(e2, m + 1, r)))

    def prolong_even(m):
        over_rows(
            *late_rows,
            lambda r: put(u2, 2 * m + 1, r, at(u1, 2 * m + 1, r) + 0.5 * (at(e2, m, r) + at(e2, m + 1, r))),
        )

    def last_residual(n):
        def chunk(r):
            v, s = with_sum(u3, n + 1, r)
            rest = at(src, n, r) + (at(u3, n, r) - v)
            res[n, :, pl.ds(r - TOP, CHUNK), :] = rest - at(coef, COND, r) * (4.0 * v - s)

        over_rows(TOP, end, chunk)

    def clear(low):
        zeros = jnp.zeros((blocks, HALO, LANES), jnp.float32)

        def planes(buf, a, b):
            for n in range(a, b):
                buf[n, :, pl.ds(low, HALO), :] = zeros

        planes(gue, 0, steps + 1)
        planes(src, 0, steps)
        planes(coef, COND, COND + 1)
        for buf in (sums, e0, e1, e2):
            planes(buf, 0, 1)

    @pl.when(top)
    def _():
        clear(TOP - HALO)

    @pl.when(bottom)
    def _():
        clear(end)

    @pl.when(first)
    def _():
        for buf in (sums, e0, e1, e2):
            buf[0, :, pl.ds(TOP, rows), :] = jnp.zeros((blocks, rows, LANES), jnp.float32)

    load_wait(0)
    x_send(0)
    h_send(0, 0, 1)
    load_wait(1)
    over_rows(TOP, end, lambda r: put(sums, 1, r, at(src, steps - 1, r) + at(gue, steps - 1, r)))
    h_send(0, 1)
    x_send(1)
    load_wait(2)
    h_send(1)
    load_wait(3)
    h_send(2)
    load_wait(4)
    h_send(3)

    def coefficients(r):
        c = at(coef, COND, r)
        inv = 1.0 / (1.0 + 4.0 * c)
        invk = 1.0 / (1.0 + 8.0 * c)
        put(coef, INV, r, inv)
        put(coef, W, r, c * inv)
        put(coef, INVK, r, invk)
        put(coef, WK, r, (2.0 * c) * invk)

    h_wait(0)
    over_rows(*fine_rows, coefficients)
    fine_smooth(gue, u1, steps - 1, steps, fine_rows)
    h_wait(1)
    fine_smooth(gue, u1, steps - 3, steps - 1, fine_rows)
    x_relay(1)
    restrict(half - 1)
    coarse_first(half - 1)
    x_send(2)
    x_edges(0)
    h_send(OLD_GUESS)
    x_relay(0)
    h_wait(2)
    fine_smooth(gue, u1, steps - 5, steps - 3, fine_rows)
    restrict(half - 2)
    coarse_first(half - 2)
    coarse_sweep(e0, e1, half - 1, 0)
    x_send_edges(3)
    x_edges(1)
    h_send(OLD_SUM)
    h_wait(3)
    fine_smooth(gue, u1, 1, steps - 5, fine_rows)
    restrict(half - 3)
    coarse_first(half - 3)
    coarse_sweep(e0, e1, half - 2, 1)
    coarse_sweep(e1, e2, half - 1, 2)
    x_send_edges(4)
    x_send_inner(3, 4)
    x_edges(2)
    h_send(OLD_E0)
    h_wait(OLD_GUESS)
    x_inner(0)
    fine_smooth(gue, u1, 0, 1, fine_rows)
    x_relay(2)

    h_wait(OLD_SUM)
    x_inner(1)
    smooth_before()
    restrict(0)
    coarse_first(0)
    x_edges(3)
    h_send(OLD_E1)
    coarse_sweep(e0, e1, 1, 3)
    coarse_sweep(e1, e2, 2, 4)
    x_relay(3)
    prolong_odd(half - 1)
    prolong_even(half - 1)
    fine_smooth(u2, u3, steps - 1, steps, late_rows)
    x_send(5)
    x_edges(4)
    h_send(OLD_E2)
    prolong_odd(half - 2)
    fine_smooth(u2, u3, steps - 2, steps - 1, late_rows)
    last_residual(steps - 1)
    h_wait(OLD_E0)
    x_inner(2)
    coarse_sweep(e0, e1, 0, 5)
    coarse_sweep(e1, e2, 1, 6)
    x_relay(4)
    prolong_even(half - 2)
    prolong_odd(half - 3)
    fine_smooth(u2, u3, steps - 4, steps - 2, late_rows)
    h_wait(OLD_E1)
    x_inner(3)
    coarse_sweep(e1, e2, 0, 7)
    over_planes(steps - 3, steps - 1, last_residual)
    prolong_even(1)
    prolong_odd(0)
    fine_smooth(u2, u3, 2, steps - 4, late_rows)
    x_relay(5)
    over_planes(3, steps - 3, last_residual)
    h_wait(OLD_E2)
    x_inner(4)
    over_rows(*late_rows, lambda r: put(u2, 0, r, at(u1, 0, r) + at(e2, 0, r)))
    prolong_even(0)
    fine_smooth(u2, u3, 0, 2, late_rows)
    over_planes(1, 3, last_residual)
    x_edges(5)
    x_inner(5)
    last_residual(0)

    @pl.when(~last)
    def _():
        rows_wait(xs, rows * len(x_plan))

    for device, jobs in relays.items():

        @pl.when(tm == device)
        def _():
            for slot, _ in jobs:
                rows_wait(fs.at[slot], sum(AROUND))

    all_rows = sum(h_rows(group) for group in h_plan)

    @pl.when(~bottom)
    def _():
        rows_wait(hs.at[0], all_rows)

    @pl.when(~top)
    def _():
        rows_wait(hs.at[1], all_rows)


def store_kernel(steps, rows, blocks, u3, res, field_out, res_out, sem):
    for k in range(blocks):
        cols = pl.ds(k * LANES, LANES)
        own = u3.at[pl.ds(1, steps), k, pl.ds(TOP, rows), :]
        pltpu.make_async_copy(own, field_out.at[:, :, cols], sem.at[0]).start()
        pltpu.make_async_copy(res.at[:, k, :, :], res_out.at[:, :, cols], sem.at[1]).start()
    pltpu.make_async_copy(field_out, field_out, sem.at[0]).wait()
    pltpu.make_async_copy(res_out, res_out, sem.at[1]).wait()


def shards(source, guess, start_state, conduct):
    steps, rows, cols = source.shape
    blocks = cols // LANES
    half = steps // 2
    tall = rows + 2 * TOP
    f32 = jnp.float32
    hbm = pl.BlockSpec(memory_space=pltpu.HBM)
    vmem = pl.BlockSpec(memory_space=pltpu.VMEM)

    def planes(n):
        return pltpu.VMEM((n, blocks, tall, LANES), f32)

    u3, res = pl.pallas_call(
        functools.partial(cycle_kernel, steps, rows, blocks),
        out_shape=(
            jax.ShapeDtypeStruct((steps + 1, blocks, tall, LANES), f32),
            jax.ShapeDtypeStruct((steps, blocks, rows, LANES), f32),
        ),
        in_specs=[hbm] * 4,
        out_specs=(vmem, vmem),
        scratch_shapes=[
            planes(steps),
            planes(steps + 1),
            planes(steps + 1),
            planes(steps + 1),
            planes(half + 1),
            planes(half + 1),
            planes(half + 1),
            planes(half),
            planes(steps),
            planes(5),
            planes(2),
            pltpu.VMEM((2, 6, blocks, max(AROUND), LANES), f32),
            pltpu.SemaphoreType.DMA((7,)),
            pltpu.SemaphoreType.DMA,
            pltpu.SemaphoreType.DMA((6, 2)),
            pltpu.SemaphoreType.DMA((2, 6)),
            pltpu.SemaphoreType.DMA((2,)),
            pltpu.SemaphoreType.DMA((2,)),
            pltpu.SemaphoreType.DMA((9, 2)),
        ],
        compiler_params=pltpu.CompilerParams(
            collective_id=0, has_side_effects=True, vmem_limit_bytes=44 * 1024 * 1024
        ),
        name="cycle",
    )(*(pltpu.with_memory_space_constraint(a, pltpu.HBM) for a in (source, guess, start_state, conduct)))
    return pl.pallas_call(
        functools.partial(store_kernel, steps, rows, blocks),
        out_shape=(jax.ShapeDtypeStruct(source.shape, f32), jax.ShapeDtypeStruct(source.shape, f32)),
        in_specs=[vmem, vmem],
        out_specs=(hbm, hbm),
        scratch_shapes=[pltpu.SemaphoreType.DMA((2,))],
        compiler_params=pltpu.CompilerParams(vmem_limit_bytes=16 * 1024 * 1024),
        name="store",
    )(u3, res)


def solution(mesh):
    return jax.shard_map(
        shards,
        mesh=mesh,
        in_specs=(
            P("tm", "space", None),
            P("tm", "space", None),
            P("space", None),
            P("space", None),
        ),
        out_specs=(P("tm", "space", None), P("tm", "space", None)),
        check_vma=False,
    )
```

```python
import functools

import jax
import jax.numpy as jnp
from jax import lax
from jax.experimental import pallas as pl
from jax.experimental.pallas import tpu as pltpu
from jax.sharding import PartitionSpec as P

damping = 0.8
MESH = pl.DeviceIdType.MESH
LANES = 128
HALO = 12
TOP = 16
CHUNK = 8
EDGE = (12, 12, 8, 8, 8, 8)
AROUND = (8, 16, 8, 12, 16, 16)


def cycle_kernel(
    steps,
    rows,
    blocks,
    source_hbm,
    guess_hbm,
    start_hbm,
    cond_hbm,
    u3,
    res,
    src,
    gue,
    u1,
    u2,
    e0,
    e1,
    e2,
    rhs,
    tmp,
    coef,
    sums,
    relay,
    load_sem,
    xs,
    xr,
    lr,
    fs,
    meet,
    hs,
    hr,
):
    half = steps // 2
    end = TOP + rows
    tm, sp = lax.axis_index("tm"), lax.axis_index("space")
    n_tm, n_sp = lax.axis_size("tm"), lax.axis_size("space")
    first, last = tm == 0, tm == n_tm - 1
    top, bottom = sp == 0, sp == n_sp - 1
    COND, INV, W, INVK, WK = range(5)

    barrier = pltpu.get_barrier_semaphore()

    def greet(cond, axis, index):
        @pl.when(cond)
        def _():
            pl.semaphore_signal(barrier, inc=1, device_id={axis: index}, device_id_type=MESH)

    greet(~first, "tm", tm - 1)
    greet(~last, "tm", tm + 1)
    greet(~top, "space", sp - 1)
    greet(~bottom, "space", sp + 1)

    def rows_wait(sem, count):
        planes = next(n for n in range(1, count + 1) if count % n == 0 and count // n <= end)
        there = gue.at[pl.ds(0, planes), :, pl.ds(0, count // planes), :]
        pltpu.make_async_copy(there, there, sem).wait()

    def load(group, hbm, lead, buf, at, count):
        out = []
        for k in range(blocks):
            cols = pl.ds(k * LANES, LANES)
            view = hbm.at[:, cols] if lead is None else hbm.at[pl.ds(lead, count), :, cols]
            dst = buf.at[at, k, pl.ds(TOP, rows), :] if lead is None else buf.at[pl.ds(at, count), k, pl.ds(TOP, rows), :]
            out.append(pltpu.make_async_copy(view, dst, load_sem.at[group]))
        return out

    def guess_load(group, low, count):
        return load(group, guess_hbm, low, gue, low + 1, count)

    def source_load(group, low, count):
        return load(group, source_hbm, low, src, low, count)

    def load_wait(group):
        rows_wait(load_sem.at[group], rows * (2, 2, 4, 4, 5, 1, 1)[group])

    for copies in (
        guess_load(0, steps - 2, 2),
        load(1, cond_hbm, None, coef, COND, 1),
        source_load(1, steps - 1, 1),
        guess_load(2, steps - 4, 2),
        source_load(2, steps - 3, 2),
        guess_load(3, steps - 6, 2),
        source_load(3, steps - 5, 2),
        guess_load(4, 0, 2),
        source_load(4, 0, 3),
    ):
        for c in copies:
            c.start()

    @pl.when(first)
    def _():
        for i, buf in enumerate((gue, u3)):
            for c in load(5 + i, start_hbm, None, buf, 0, 1):
                c.start()

    one = jnp.int32(1)
    zero = jnp.int32(0)
    peers = [jnp.where(edge, zero, one) for edge in (first, last, top, bottom)]
    pl.semaphore_wait(barrier, peers[0] + peers[1] + peers[2] + peers[3])

    x_plan = [(gue, steps), (sums, 1), (e0, half), (e1, half), (e2, half), (u3, steps)]
    ways = {0: (3, 0), 1: (3, 1), 2: (1, 0)}
    relays = {3: ((0, 1), (1, 2)), 1: ((0, 3),)}
    FIRST_ROWS, LAST_ROWS, INNER, AROUND_ROWS = range(4)

    def part(i, piece):
        edge, inner = EDGE[i], rows - 2 * EDGE[i] - AROUND[i]
        return pl.ds(
            *((TOP, edge), (end - edge, edge), (TOP + edge, inner), (TOP + edge + inner, AROUND[i]))[piece]
        )

    def x_copy(i, piece):
        buf, plane = x_plan[i]
        return pltpu.make_async_remote_copy(
            src_ref=buf.at[plane, :, part(i, piece), :],
            dst_ref=buf.at[0, :, part(i, piece), :],
            send_sem=xs,
            recv_sem=xr.at[i, piece // 2],
            device_id={"tm": tm + 1},
            device_id_type=MESH,
        )

    def to_relay(i, device, slot):
        buf, plane = x_plan[i]
        return pltpu.make_async_remote_copy(
            src_ref=buf.at[plane, :, part(i, AROUND_ROWS), :],
            dst_ref=relay.at[slot, i, :, pl.ds(0, AROUND[i]), :],
            send_sem=xs,
            recv_sem=lr.at[slot, i],
            device_id={"tm": device},
            device_id_type=MESH,
        )

    def from_relay(i, slot, device):
        return pltpu.make_async_remote_copy(
            src_ref=relay.at[slot, i, :, pl.ds(0, AROUND[i]), :],
            dst_ref=x_plan[i][0].at[0, :, part(i, AROUND_ROWS), :],
            send_sem=fs.at[slot],
            recv_sem=xr.at[i, 1],
            device_id={"tm": device},
            device_id_type=MESH,
        )

    def x_send_edges(i):
        @pl.when(~last)
        def _():
            x_copy(i, FIRST_ROWS).start()
            x_copy(i, LAST_ROWS).start()

    def x_send_around(i):
        for sender, way in ways.items():

            @pl.when(tm == sender)
            def _():
                to_relay(i, *way).start()

    def x_send_inner(*which):
        @pl.when(~last)
        def _():
            for i in which:
                x_copy(i, INNER).start()

    def x_tell(device):
        @pl.when(tm == device)
        def _():
            pl.semaphore_signal(meet, inc=1, device_id={"tm": device - 1}, device_id_type=MESH)

    def x_hear(device):
        @pl.when(tm == device)
        def _():
            pl.semaphore_wait(meet, 1)

    def x_send(i):
        x_send_edges(i)
        x_send_around(i)
        x_send_inner(i)

    def x_relay(i):
        for device, jobs in relays.items():

            @pl.when(tm == device)
            def _():
                for slot, final in jobs:
                    to_relay(i, device, slot).wait_recv()
                    from_relay(i, slot, final).start()

    def x_edges(i):
        @pl.when(~first)
        def _():
            rows_wait(xr.at[i, 0], 2 * EDGE[i])

        if i in (0, 5):

            @pl.when(first)
            def _():
                load_wait(5 if i == 0 else 6)

    def x_inner(i):
        @pl.when(~first)
        def _():
            rows_wait(xr.at[i, 1], rows - 2 * EDGE[i])

    h_plan = [
        ((gue, steps - 1, 2, 11), (coef, COND, 1, 10), (src, steps - 1, 1, 10)),
        ((gue, steps - 3, 2, 11), (src, steps - 3, 2, 10)),
        ((gue, steps - 5, 2, 11), (src, steps - 5, 2, 10)),
        ((gue, 1, 2, 11), (src, 0, 3, 10)),
        ((gue, 0, 1, 10),),
        ((sums, 0, 1, 9),),
        ((e0, 0, 1, 6),),
        ((e1, 0, 1, 4),),
        ((e2, 0, 1, 3),),
    ]
    OLD_GUESS, OLD_SUM, OLD_E0, OLD_E1, OLD_E2 = range(4, 9)

    def down_copy(i, buf, plane, count, width):
        return pltpu.make_async_remote_copy(
            src_ref=buf.at[pl.ds(plane, count), :, pl.ds(end - width, width), :],
            dst_ref=buf.at[pl.ds(plane, count), :, pl.ds(TOP - width, width), :],
            send_sem=hs.at[0],
            recv_sem=hr.at[i, 0],
            device_id={"space": sp + 1},
            device_id_type=MESH,
        )

    def up_copy(i, buf, plane, count, width):
        return pltpu.make_async_remote_copy(
            src_ref=buf.at[pl.ds(plane, count), :, pl.ds(TOP, width), :],
            dst_ref=buf.at[pl.ds(plane, count), :, pl.ds(end, width), :],
            send_sem=hs.at[1],
            recv_sem=hr.at[i, 1],
            device_id={"space": sp - 1},
            device_id_type=MESH,
        )

    def h_send(i, low=0, high=9):
        @pl.when(~bottom)
        def _():
            for item in h_plan[i][low:high]:
                down_copy(i, *item).start()

        @pl.when(~top)
        def _():
            for item in h_plan[i][low:high]:
                up_copy(i, *item).start()

    def h_rows(group):
        return sum(count * width for _, _, count, width in group)

    def h_wait(i):
        @pl.when(~top)
        def _():
            rows_wait(hr.at[i, 0], h_rows(h_plan[i]))

        @pl.when(~bottom)
        def _():
            rows_wait(hr.at[i, 1], h_rows(h_plan[i]))

    def at(buf, n, r):
        return buf[n, :, pl.ds(r, CHUNK), :]

    def put(buf, n, r, value):
        buf[n, :, pl.ds(r, CHUNK), :] = value

    def sideways(v):
        lane = lax.broadcasted_iota(jnp.int32, v.shape, 2)
        edge = jnp.zeros((1,) + v.shape[1:], jnp.float32)
        fwd = pltpu.roll(v, 1, 2)
        bwd = pltpu.roll(v, LANES - 1, 2)
        left = jnp.where(lane == 0, jnp.concatenate([edge, fwd[:-1]], axis=0), fwd)
        right = jnp.where(lane == LANES - 1, jnp.concatenate([bwd[1:], edge], axis=0), bwd)
        return left + right

    def with_sum(buf, n, r):
        v = at(buf, n, r)
        return v, (at(buf, n, r - 1) + at(buf, n, r + 1)) + sideways(v)

    def over_rows(low, high, body):
        count = (high - low) // CHUNK

        def step(i, carry):
            body(low + i * CHUNK)
            return carry

        lax.fori_loop(0, count, step, 0, unroll=True)

    def over_planes(low, high, body):
        if high - low == 1:
            body(low)
        else:

            def step(i, carry):
                body(i)
                return carry

            lax.fori_loop(low, high, step, 0)

    def grown(extra):
        return (TOP - extra, end + extra)

    fine_rows, coarse_rows, late_rows = grown(12), grown(8), grown(4)

    def fine_smooth(frm, to, low, high, where):
        def first_pass(n):
            def chunk(r):
                v, s = with_sum(frm, n + 1, r)
                rest = at(src, n, r) + at(frm, n, r)
                put(tmp, n, r, damping * (at(coef, INV, r) * rest + at(coef, W, r) * s - v))

            over_rows(*where, chunk)

        def second_pass(n):
            def chunk(r):
                v, s = with_sum(tmp, n, r)
                put(to, n + 1, r, at(frm, n + 1, r) + (v + at(coef, W, r) * s))

            over_rows(*where, chunk)

        over_planes(low, high, first_pass)
        over_planes(low, high, second_pass)

    def smooth_before():
        def first_pass(r):
            v, s = with_sum(gue, 0, r)
            put(tmp, 0, r, damping * (at(coef, INV, r) * at(sums, 0, r) + at(coef, W, r) * s - v))

        def second_pass(r):
            v, s = with_sum(tmp, 0, r)
            put(u1, 0, r, at(gue, 0, r) + (v + at(coef, W, r) * s))

        @pl.when(first)
        def _():
            over_rows(*fine_rows, lambda r: put(u1, 0, r, at(gue, 0, r)))

        @pl.when(~first)
        def _():
            over_rows(*fine_rows, first_pass)
            over_rows(*fine_rows, second_pass)

    def restrict(m):
        def chunk(r):
            a, sa = at(u1, 2 * m + 1, r), at(u1, 2 * m + 1, r - 1) + at(u1, 2 * m + 1, r + 1)
            b, sb = at(u1, 2 * m + 2, r), at(u1, 2 * m + 2, r - 1) + at(u1, 2 * m + 2, r + 1)
            pair = a + b
            around = (sa + sb) + sideways(pair)
            total = at(src, 2 * m, r) + at(src, 2 * m + 1, r) + (at(u1, 2 * m, r) - b)
            total = total - at(coef, COND, r) * (4.0 * pair - around)
            put(rhs, m, r, at(coef, INVK, r) * total)

        over_rows(*coarse_rows, chunk)

    def coarse_first(m):
        def chunk(r):
            v, s = with_sum(rhs, m, r)
            put(e0, m + 1, r, damping * (v + at(coef, WK, r) * s))

        over_rows(*coarse_rows, chunk)

    def coarse_sweep(frm, to, m, slot):
        def first_pass(r):
            v, s = with_sum(frm, m + 1, r)
            rest = at(rhs, m, r) + at(coef, INVK, r) * at(frm, m, r)
            put(tmp, slot, r, damping * (rest + at(coef, WK, r) * s - v))

        def second_pass(r):
            v, s = with_sum(tmp, slot, r)
            put(to, m + 1, r, at(frm, m + 1, r) + (v + at(coef, WK, r) * s))

        where = late_rows if to is e2 else coarse_rows
        over_rows(*where, first_pass)
        over_rows(*where, second_pass)

    def prolong_odd(m):
        over_rows(*late_rows, lambda r: put(u2, 2 * m + 2, r, at(u1, 2 * m + 2, r) + at(e2, m + 1, r)))

    def prolong_even(m):
        over_rows(
            *late_rows,
            lambda r: put(u2, 2 * m + 1, r, at(u1, 2 * m + 1, r) + 0.5 * (at(e2, m, r) + at(e2, m + 1, r))),
        )

    def last_residual(n):
        def chunk(r):
            v, s = with_sum(u3, n + 1, r)
            rest = at(src, n, r) - v if isinstance(n, int) and n == 0 else at(src, n, r) + (at(u3, n, r) - v)
            res[n, :, pl.ds(r - TOP, CHUNK), :] = rest - at(coef, COND, r) * (4.0 * v - s)

        over_rows(TOP, end, chunk)

    def clear(low):
        zeros = jnp.zeros((blocks, HALO, LANES), jnp.float32)

        def planes(buf, a, b):
            for n in range(a, b):
                buf[n, :, pl.ds(low, HALO), :] = zeros

        planes(gue, 0, steps + 1)
        planes(src, 0, steps)
        planes(coef, COND, COND + 1)
        for buf in (sums, e0, e1, e2):
            planes(buf, 0, 1)

    @pl.when(top)
    def _():
        clear(TOP - HALO)

    @pl.when(bottom)
    def _():
        clear(end)

    @pl.when(first)
    def _():
        for buf in (sums, e0, e1, e2):
            buf[0, :, pl.ds(TOP, rows), :] = jnp.zeros((blocks, rows, LANES), jnp.float32)

    x_tell(2)
    load_wait(0)
    x_send_edges(0)
    x_send_inner(0)
    h_send(0, 0, 1)
    load_wait(1)
    over_rows(TOP, end, lambda r: put(sums, 1, r, at(src, steps - 1, r) + at(gue, steps - 1, r)))
    h_send(0, 1)
    x_send_edges(1)
    x_send_inner(1)
    x_hear(1)
    x_tell(1)
    load_wait(2)
    h_send(1)
    load_wait(3)
    h_send(2)
    load_wait(4)
    h_send(3)
    x_hear(0)
    x_send_around(1)
    x_send_around(0)

    def coefficients(r):
        c = at(coef, COND, r)
        inv = 1.0 / (1.0 + 4.0 * c)
        invk = 1.0 / (1.0 + 8.0 * c)
        put(coef, INV, r, inv)
        put(coef, W, r, c * inv)
        put(coef, INVK, r, invk)
        put(coef, WK, r, (2.0 * c) * invk)

    h_wait(0)
    over_rows(*fine_rows, coefficients)
    fine_smooth(gue, u1, steps - 1, steps, fine_rows)
    h_wait(1)
    fine_smooth(gue, u1, steps - 3, steps - 1, fine_rows)
    x_relay(1)
    restrict(half - 1)
    coarse_first(half - 1)
    x_send(2)
    x_edges(0)
    h_send(OLD_GUESS)
    x_relay(0)
    h_wait(2)
    fine_smooth(gue, u1, steps - 5, steps - 3, fine_rows)
    restrict(half - 2)
    coarse_first(half - 2)
    coarse_sweep(e0, e1, half - 1, 0)
    x_send_edges(3)
    x_send_around(3)
    x_edges(1)
    h_send(OLD_SUM)
    h_wait(3)
    fine_smooth(gue, u1, 1, steps - 5, fine_rows)
    restrict(half - 3)
    coarse_first(half - 3)
    coarse_sweep(e0, e1, half - 2, 1)
    coarse_sweep(e1, e2, half - 1, 2)
    x_send_edges(4)
    x_send_around(4)
    x_send_inner(3, 4)
    x_edges(2)
    h_send(OLD_E0)
    h_wait(OLD_GUESS)
    x_inner(0)
    fine_smooth(gue, u1, 0, 1, fine_rows)
    x_relay(2)

    h_wait(OLD_SUM)
    x_inner(1)
    smooth_before()
    restrict(0)
    coarse_first(0)
    x_edges(3)
    h_send(OLD_E1)
    x_relay(3)
    coarse_sweep(e0, e1, 1, 3)
    coarse_sweep(e1, e2, 2, 4)
    prolong_odd(half - 1)
    prolong_even(half - 1)
    fine_smooth(u2, u3, steps - 1, steps, late_rows)
    x_send(5)
    x_edges(4)
    h_send(OLD_E2)
    prolong_odd(half - 2)
    fine_smooth(u2, u3, steps - 2, steps - 1, late_rows)
    last_residual(steps - 1)
    h_wait(OLD_E0)
    x_inner(2)
    coarse_sweep(e0, e1, 0, 5)
    coarse_sweep(e1, e2, 1, 6)
    x_relay(4)
    prolong_even(half - 2)
    prolong_odd(half - 3)
    fine_smooth(u2, u3, steps - 4, steps - 2, late_rows)
    h_wait(OLD_E1)
    x_inner(3)
    coarse_sweep(e1, e2, 0, 7)
    over_planes(steps - 3, steps - 1, last_residual)
    x_relay(5)
    prolong_even(1)
    prolong_odd(0)
    fine_smooth(u2, u3, 2, steps - 4, late_rows)
    over_planes(3, steps - 3, last_residual)
    h_wait(OLD_E2)
    x_inner(4)
    over_rows(*late_rows, lambda r: put(u2, 0, r, at(u1, 0, r) + at(e2, 0, r)))
    prolong_even(0)
    fine_smooth(u2, u3, 0, 2, late_rows)
    over_planes(1, 3, last_residual)
    last_residual(0)
    x_edges(5)
    x_inner(5)

    def add_before(r):
        part = pl.ds(r - TOP, CHUNK)
        res[0, :, part, :] = res[0, :, part, :] + at(u3, 0, r)

    over_rows(TOP, end, add_before)

    @pl.when(~last)
    def _():
        rows_wait(xs, rows * len(x_plan))

    for device, jobs in relays.items():

        @pl.when(tm == device)
        def _():
            for slot, _ in jobs:
                rows_wait(fs.at[slot], sum(AROUND))

    all_rows = sum(h_rows(group) for group in h_plan)

    @pl.when(~bottom)
    def _():
        rows_wait(hs.at[0], all_rows)

    @pl.when(~top)
    def _():
        rows_wait(hs.at[1], all_rows)


def store_kernel(steps, rows, blocks, u3, res, field_out, res_out, sem):
    for k in range(blocks):
        cols = pl.ds(k * LANES, LANES)
        own = u3.at[pl.ds(1, steps), k, pl.ds(TOP, rows), :]
        pltpu.make_async_copy(own, field_out.at[:, :, cols], sem.at[0]).start()
        pltpu.make_async_copy(res.at[:, k, :, :], res_out.at[:, :, cols], sem.at[1]).start()
    pltpu.make_async_copy(field_out, field_out, sem.at[0]).wait()
    pltpu.make_async_copy(res_out, res_out, sem.at[1]).wait()


def shards(source, guess, start_state, conduct):
    steps, rows, cols = source.shape
    blocks = cols // LANES
    half = steps // 2
    tall = rows + 2 * TOP
    f32 = jnp.float32
    hbm = pl.BlockSpec(memory_space=pltpu.HBM)
    vmem = pl.BlockSpec(memory_space=pltpu.VMEM)

    def planes(n):
        return pltpu.VMEM((n, blocks, tall, LANES), f32)

    u3, res = pl.pallas_call(
        functools.partial(cycle_kernel, steps, rows, blocks),
        out_shape=(
            jax.ShapeDtypeStruct((steps + 1, blocks, tall, LANES), f32),
            jax.ShapeDtypeStruct((steps, blocks, rows, LANES), f32),
        ),
        in_specs=[hbm] * 4,
        out_specs=(vmem, vmem),
        scratch_shapes=[
            planes(steps),
            planes(steps + 1),
            planes(steps + 1),
            planes(steps + 1),
            planes(half + 1),
            planes(half + 1),
            planes(half + 1),
            planes(half),
            planes(steps),
            planes(5),
            planes(2),
            pltpu.VMEM((2, 6, blocks, max(AROUND), LANES), f32),
            pltpu.SemaphoreType.DMA((7,)),
            pltpu.SemaphoreType.DMA,
            pltpu.SemaphoreType.DMA((6, 2)),
            pltpu.SemaphoreType.DMA((2, 6)),
            pltpu.SemaphoreType.DMA((2,)),
            pltpu.SemaphoreType.REGULAR,
            pltpu.SemaphoreType.DMA((2,)),
            pltpu.SemaphoreType.DMA((9, 2)),
        ],
        compiler_params=pltpu.CompilerParams(
            collective_id=0, has_side_effects=True, vmem_limit_bytes=44 * 1024 * 1024
        ),
        name="cycle",
    )(*(pltpu.with_memory_space_constraint(a, pltpu.HBM) for a in (source, guess, start_state, conduct)))
    return pl.pallas_call(
        functools.partial(store_kernel, steps, rows, blocks),
        out_shape=(jax.ShapeDtypeStruct(source.shape, f32), jax.ShapeDtypeStruct(source.shape, f32)),
        in_specs=[vmem, vmem],
        out_specs=(hbm, hbm),
        scratch_shapes=[pltpu.SemaphoreType.DMA((2,))],
        compiler_params=pltpu.CompilerParams(vmem_limit_bytes=16 * 1024 * 1024),
        name="store",
    )(u3, res)


def solution(mesh):
    return jax.shard_map(
        shards,
        mesh=mesh,
        in_specs=(
            P("tm", "space", None),
            P("tm", "space", None),
            P("space", None),
            P("space", None),
        ),
        out_specs=(P("tm", "space", None), P("tm", "space", None)),
        check_vma=False,
    )
```

```python
import functools

import jax
import jax.numpy as jnp
from jax import lax
from jax.experimental import pallas as pl
from jax.experimental.pallas import tpu as pltpu
from jax.sharding import PartitionSpec as P

damping = 0.8
MESH = pl.DeviceIdType.MESH
LANES = 128
HALO = 12
TOP = 16
CHUNK = 8
EDGE = (12, 12, 8, 8, 8, 8)
AROUND = (8, 16, 8, 12, 16, 12)


def cycle_kernel(
    steps,
    rows,
    blocks,
    source_hbm,
    guess_hbm,
    start_hbm,
    cond_hbm,
    u3,
    res,
    src,
    gue,
    u1,
    u2,
    e0,
    e1,
    e2,
    rhs,
    tmp,
    coef,
    sums,
    relay,
    load_sem,
    xs,
    xr,
    lr,
    fs,
    meet,
    hs,
    hr,
):
    half = steps // 2
    end = TOP + rows
    tm, sp = lax.axis_index("tm"), lax.axis_index("space")
    n_tm, n_sp = lax.axis_size("tm"), lax.axis_size("space")
    first, last = tm == 0, tm == n_tm - 1
    top, bottom = sp == 0, sp == n_sp - 1
    COND, INV, W, INVK, WK = range(5)

    barrier = pltpu.get_barrier_semaphore()

    def greet(cond, axis, index):
        @pl.when(cond)
        def _():
            pl.semaphore_signal(barrier, inc=1, device_id={axis: index}, device_id_type=MESH)

    greet(~first, "tm", tm - 1)
    greet(~last, "tm", tm + 1)
    greet(~top, "space", sp - 1)
    greet(~bottom, "space", sp + 1)

    def rows_wait(sem, count):
        planes = next(n for n in range(1, count + 1) if count % n == 0 and count // n <= end)
        there = gue.at[pl.ds(0, planes), :, pl.ds(0, count // planes), :]
        pltpu.make_async_copy(there, there, sem).wait()

    def load(group, hbm, lead, buf, at, count):
        out = []
        for k in range(blocks):
            cols = pl.ds(k * LANES, LANES)
            view = hbm.at[:, cols] if lead is None else hbm.at[pl.ds(lead, count), :, cols]
            dst = buf.at[at, k, pl.ds(TOP, rows), :] if lead is None else buf.at[pl.ds(at, count), k, pl.ds(TOP, rows), :]
            out.append(pltpu.make_async_copy(view, dst, load_sem.at[group]))
        return out

    def guess_load(group, low, count):
        return load(group, guess_hbm, low, gue, low + 1, count)

    def source_load(group, low, count):
        return load(group, source_hbm, low, src, low, count)

    def load_wait(group):
        rows_wait(load_sem.at[group], rows * (2, 2, 4, 4, 5, 1, 1)[group])

    for copies in (
        guess_load(0, steps - 2, 2),
        load(1, cond_hbm, None, coef, COND, 1),
        source_load(1, steps - 1, 1),
        guess_load(2, steps - 4, 2),
        source_load(2, steps - 3, 2),
        guess_load(3, steps - 6, 2),
        source_load(3, steps - 5, 2),
        guess_load(4, 0, 2),
        source_load(4, 0, 3),
    ):
        for c in copies:
            c.start()

    @pl.when(first)
    def _():
        for i, buf in enumerate((gue, u3)):
            for c in load(5 + i, start_hbm, None, buf, 0, 1):
                c.start()

    one = jnp.int32(1)
    zero = jnp.int32(0)
    peers = [jnp.where(edge, zero, one) for edge in (first, last, top, bottom)]
    pl.semaphore_wait(barrier, peers[0] + peers[1] + peers[2] + peers[3])

    x_plan = [(gue, steps), (sums, 1), (e0, half), (e1, half), (e2, half), (u3, steps)]
    ways = {0: (3, 0), 1: (3, 1), 2: (1, 0)}
    relays = {3: ((0, 1), (1, 2)), 1: ((0, 3),)}
    FIRST_ROWS, LAST_ROWS, INNER, AROUND_ROWS = range(4)

    def part(i, piece):
        edge, inner = EDGE[i], rows - 2 * EDGE[i] - AROUND[i]
        return pl.ds(
            *((TOP, edge), (end - edge, edge), (TOP + edge, inner), (TOP + edge + inner, AROUND[i]))[piece]
        )

    def x_copy(i, piece):
        buf, plane = x_plan[i]
        return pltpu.make_async_remote_copy(
            src_ref=buf.at[plane, :, part(i, piece), :],
            dst_ref=buf.at[0, :, part(i, piece), :],
            send_sem=xs,
            recv_sem=xr.at[i, piece // 2],
            device_id={"tm": tm + 1},
            device_id_type=MESH,
        )

    def to_relay(i, device, slot):
        buf, plane = x_plan[i]
        return pltpu.make_async_remote_copy(
            src_ref=buf.at[plane, :, part(i, AROUND_ROWS), :],
            dst_ref=relay.at[slot, i, :, pl.ds(0, AROUND[i]), :],
            send_sem=xs,
            recv_sem=lr.at[slot, i],
            device_id={"tm": device},
            device_id_type=MESH,
        )

    def from_relay(i, slot, device):
        return pltpu.make_async_remote_copy(
            src_ref=relay.at[slot, i, :, pl.ds(0, AROUND[i]), :],
            dst_ref=x_plan[i][0].at[0, :, part(i, AROUND_ROWS), :],
            send_sem=fs.at[slot],
            recv_sem=xr.at[i, 1],
            device_id={"tm": device},
            device_id_type=MESH,
        )

    def x_send_edges(i):
        @pl.when(~last)
        def _():
            x_copy(i, FIRST_ROWS).start()
            x_copy(i, LAST_ROWS).start()

    def x_send_around(i):
        for sender, way in ways.items():

            @pl.when(tm == sender)
            def _():
                to_relay(i, *way).start()

    def x_send_inner(*which):
        @pl.when(~last)
        def _():
            for i in which:
                x_copy(i, INNER).start()

    def x_tell(device):
        @pl.when(tm == device)
        def _():
            pl.semaphore_signal(meet, inc=1, device_id={"tm": device - 1}, device_id_type=MESH)

    def x_hear(device):
        @pl.when(tm == device)
        def _():
            pl.semaphore_wait(meet, 1)

    def x_send(i):
        x_send_edges(i)
        x_send_around(i)
        x_send_inner(i)

    def x_relay(i):
        for device, jobs in relays.items():

            @pl.when(tm == device)
            def _():
                for slot, final in jobs:
                    to_relay(i, device, slot).wait_recv()
                    from_relay(i, slot, final).start()

    def x_edges(i):
        @pl.when(~first)
        def _():
            rows_wait(xr.at[i, 0], 2 * EDGE[i])

        if i in (0, 5):

            @pl.when(first)
            def _():
                load_wait(5 if i == 0 else 6)

    def x_inner(i):
        @pl.when(~first)
        def _():
            rows_wait(xr.at[i, 1], rows - 2 * EDGE[i])

    h_plan = [
        ((gue, steps - 1, 2, 11), (coef, COND, 1, 10), (src, steps - 1, 1, 10)),
        ((gue, steps - 3, 2, 11), (src, steps - 3, 2, 10)),
        ((gue, steps - 5, 2, 11), (src, steps - 5, 2, 10)),
        ((gue, 1, 2, 11), (src, 0, 3, 10)),
        ((gue, 0, 1, 10),),
        ((sums, 0, 1, 9),),
        ((e0, 0, 1, 6),),
        ((e1, 0, 1, 4),),
        ((e2, 0, 1, 3),),
    ]
    OLD_GUESS, OLD_SUM, OLD_E0, OLD_E1, OLD_E2 = range(4, 9)

    def down_copy(i, buf, plane, count, width):
        return pltpu.make_async_remote_copy(
            src_ref=buf.at[pl.ds(plane, count), :, pl.ds(end - width, width), :],
            dst_ref=buf.at[pl.ds(plane, count), :, pl.ds(TOP - width, width), :],
            send_sem=hs,
            recv_sem=hr.at[i],
            device_id={"space": sp + 1},
            device_id_type=MESH,
        )

    def up_copy(i, buf, plane, count, width):
        return pltpu.make_async_remote_copy(
            src_ref=buf.at[pl.ds(plane, count), :, pl.ds(TOP, width), :],
            dst_ref=buf.at[pl.ds(plane, count), :, pl.ds(end, width), :],
            send_sem=hs,
            recv_sem=hr.at[i],
            device_id={"space": sp - 1},
            device_id_type=MESH,
        )

    def h_send(i, low=0, high=9):
        @pl.when(~bottom)
        def _():
            for item in h_plan[i][low:high]:
                down_copy(i, *item).start()

        @pl.when(~top)
        def _():
            for item in h_plan[i][low:high]:
                up_copy(i, *item).start()

    def h_rows(group):
        return sum(count * width for _, _, count, width in group)

    def h_count(sem, count):
        @pl.when(top | bottom)
        def _():
            rows_wait(sem, count)

        @pl.when(~top & ~bottom)
        def _():
            rows_wait(sem, 2 * count)

    def h_wait(i):
        h_count(hr.at[i], h_rows(h_plan[i]))

    def at(buf, n, r):
        return buf[n, :, pl.ds(r, CHUNK), :]

    def put(buf, n, r, value):
        buf[n, :, pl.ds(r, CHUNK), :] = value

    def sideways(v):
        lane = lax.broadcasted_iota(jnp.int32, v.shape, 2)
        edge = jnp.zeros((1,) + v.shape[1:], jnp.float32)
        fwd = pltpu.roll(v, 1, 2)
        bwd = pltpu.roll(v, LANES - 1, 2)
        left = jnp.where(lane == 0, jnp.concatenate([edge, fwd[:-1]], axis=0), fwd)
        right = jnp.where(lane == LANES - 1, jnp.concatenate([bwd[1:], edge], axis=0), bwd)
        return left + right

    def with_sum(buf, n, r):
        v = at(buf, n, r)
        return v, (at(buf, n, r - 1) + at(buf, n, r + 1)) + sideways(v)

    def over_rows(low, high, body):
        count = (high - low) // CHUNK

        def step(i, carry):
            body(low + i * CHUNK)
            return carry

        lax.fori_loop(0, count, step, 0, unroll=True)

    def over_planes(low, high, body):
        if high - low == 1:
            body(low)
        else:

            def step(i, carry):
                body(i)
                return carry

            lax.fori_loop(low, high, step, 0)

    def grown(extra):
        return (TOP - extra, end + extra)

    fine_rows, coarse_rows, late_rows = grown(12), grown(8), grown(4)

    def fine_smooth(frm, to, low, high, where):
        def first_pass(n):
            def chunk(r):
                v, s = with_sum(frm, n + 1, r)
                rest = at(src, n, r) + at(frm, n, r)
                put(tmp, n, r, damping * (at(coef, INV, r) * rest + at(coef, W, r) * s - v))

            over_rows(*where, chunk)

        def second_pass(n):
            def chunk(r):
                v, s = with_sum(tmp, n, r)
                put(to, n + 1, r, at(frm, n + 1, r) + (v + at(coef, W, r) * s))

            over_rows(*where, chunk)

        over_planes(low, high, first_pass)
        over_planes(low, high, second_pass)

    def smooth_before():
        def first_pass(r):
            v, s = with_sum(gue, 0, r)
            put(tmp, 0, r, damping * (at(coef, INV, r) * at(sums, 0, r) + at(coef, W, r) * s - v))

        def second_pass(r):
            v, s = with_sum(tmp, 0, r)
            put(u1, 0, r, at(gue, 0, r) + (v + at(coef, W, r) * s))

        @pl.when(first)
        def _():
            over_rows(*fine_rows, lambda r: put(u1, 0, r, at(gue, 0, r)))

        @pl.when(~first)
        def _():
            over_rows(*fine_rows, first_pass)
            over_rows(*fine_rows, second_pass)

    def restrict(m):
        def chunk(r):
            a, sa = at(u1, 2 * m + 1, r), at(u1, 2 * m + 1, r - 1) + at(u1, 2 * m + 1, r + 1)
            b, sb = at(u1, 2 * m + 2, r), at(u1, 2 * m + 2, r - 1) + at(u1, 2 * m + 2, r + 1)
            pair = a + b
            around = (sa + sb) + sideways(pair)
            total = at(src, 2 * m, r) + at(src, 2 * m + 1, r) + (at(u1, 2 * m, r) - b)
            total = total - at(coef, COND, r) * (4.0 * pair - around)
            put(rhs, m, r, at(coef, INVK, r) * total)

        over_rows(*coarse_rows, chunk)

    def coarse_first(m):
        def chunk(r):
            v, s = with_sum(rhs, m, r)
            put(e0, m + 1, r, damping * (v + at(coef, WK, r) * s))

        over_rows(*coarse_rows, chunk)

    def coarse_sweep(frm, to, m, slot):
        def first_pass(r):
            v, s = with_sum(frm, m + 1, r)
            rest = at(rhs, m, r) + at(coef, INVK, r) * at(frm, m, r)
            put(tmp, slot, r, damping * (rest + at(coef, WK, r) * s - v))

        def second_pass(r):
            v, s = with_sum(tmp, slot, r)
            put(to, m + 1, r, at(frm, m + 1, r) + (v + at(coef, WK, r) * s))

        where = late_rows if to is e2 else coarse_rows
        over_rows(*where, first_pass)
        over_rows(*where, second_pass)

    def prolong_odd(m):
        over_rows(*late_rows, lambda r: put(u2, 2 * m + 2, r, at(u1, 2 * m + 2, r) + at(e2, m + 1, r)))

    def prolong_even(m):
        over_rows(
            *late_rows,
            lambda r: put(u2, 2 * m + 1, r, at(u1, 2 * m + 1, r) + 0.5 * (at(e2, m, r) + at(e2, m + 1, r))),
        )

    def last_residual(n):
        def chunk(r):
            v, s = with_sum(u3, n + 1, r)
            rest = at(src, n, r) - v if isinstance(n, int) and n == 0 else at(src, n, r) + (at(u3, n, r) - v)
            res[n, :, pl.ds(r - TOP, CHUNK), :] = rest - at(coef, COND, r) * (4.0 * v - s)

        over_rows(TOP, end, chunk)

    def clear(low):
        zeros = jnp.zeros((blocks, HALO, LANES), jnp.float32)

        def planes(buf, a, b):
            for n in range(a, b):
                buf[n, :, pl.ds(low, HALO), :] = zeros

        planes(gue, 0, steps + 1)
        planes(src, 0, steps)
        planes(coef, COND, COND + 1)
        for buf in (sums, e0, e1, e2):
            planes(buf, 0, 1)

    @pl.when(top)
    def _():
        clear(TOP - HALO)

    @pl.when(bottom)
    def _():
        clear(end)

    @pl.when(first)
    def _():
        for buf in (sums, e0, e1, e2):
            buf[0, :, pl.ds(TOP, rows), :] = jnp.zeros((blocks, rows, LANES), jnp.float32)

    odd = lax.rem(sp, 2) == 1

    def x_send_inner_if(turn, *which):
        @pl.when(turn & ~last)
        def _():
            for i in which:
                x_copy(i, INNER).start()

    x_tell(2)
    load_wait(0)
    x_send_edges(0)
    x_send_inner(0)
    h_send(0, 0, 1)
    load_wait(1)
    over_rows(TOP, end, lambda r: put(sums, 1, r, at(src, steps - 1, r) + at(gue, steps - 1, r)))
    h_send(0, 1)
    x_send_edges(1)
    x_send_inner(1)
    x_hear(1)
    x_tell(1)
    load_wait(2)
    h_send(1)
    load_wait(3)
    h_send(2)
    load_wait(4)
    h_send(3)
    x_hear(0)
    x_send_around(1)
    x_send_around(0)

    def coefficients(r):
        c = at(coef, COND, r)
        inv = 1.0 / (1.0 + 4.0 * c)
        invk = 1.0 / (1.0 + 8.0 * c)
        put(coef, INV, r, inv)
        put(coef, W, r, c * inv)
        put(coef, INVK, r, invk)
        put(coef, WK, r, (2.0 * c) * invk)

    h_wait(0)
    over_rows(*fine_rows, coefficients)
    fine_smooth(gue, u1, steps - 1, steps, fine_rows)
    h_wait(1)
    fine_smooth(gue, u1, steps - 3, steps - 1, fine_rows)
    x_relay(1)
    restrict(half - 1)
    coarse_first(half - 1)
    x_send(2)
    x_edges(0)
    h_send(OLD_GUESS)
    x_relay(0)
    h_wait(2)
    fine_smooth(gue, u1, steps - 5, steps - 3, fine_rows)
    restrict(half - 2)
    coarse_first(half - 2)
    coarse_sweep(e0, e1, half - 1, 0)
    x_send_edges(3)
    x_send_around(3)
    x_edges(1)
    h_send(OLD_SUM)
    h_wait(3)
    fine_smooth(gue, u1, 1, steps - 5, fine_rows)
    restrict(half - 3)
    coarse_first(half - 3)
    coarse_sweep(e0, e1, half - 2, 1)
    coarse_sweep(e1, e2, half - 1, 2)
    x_send_edges(4)
    x_send_around(4)
    x_send_inner_if(~odd, 3, 4)
    x_edges(2)
    h_send(OLD_E0)
    h_wait(OLD_GUESS)
    x_inner(0)
    fine_smooth(gue, u1, 0, 1, fine_rows)
    x_relay(2)

    h_wait(OLD_SUM)
    x_inner(1)
    smooth_before()
    restrict(0)
    coarse_first(0)
    x_send_inner_if(odd, 3, 4)
    x_edges(3)
    h_send(OLD_E1)
    x_relay(3)
    coarse_sweep(e0, e1, 1, 3)
    coarse_sweep(e1, e2, 2, 4)
    prolong_odd(half - 1)
    prolong_even(half - 1)
    fine_smooth(u2, u3, steps - 1, steps, late_rows)
    x_send(5)
    x_edges(4)
    h_send(OLD_E2)
    prolong_odd(half - 2)
    fine_smooth(u2, u3, steps - 2, steps - 1, late_rows)
    last_residual(steps - 1)
    h_wait(OLD_E0)
    x_inner(2)
    coarse_sweep(e0, e1, 0, 5)
    coarse_sweep(e1, e2, 1, 6)
    x_relay(4)
    prolong_even(half - 2)
    prolong_odd(half - 3)
    fine_smooth(u2, u3, steps - 4, steps - 2, late_rows)
    h_wait(OLD_E1)
    x_inner(3)
    coarse_sweep(e1, e2, 0, 7)
    over_planes(steps - 3, steps - 1, last_residual)
    x_relay(5)
    prolong_even(1)
    prolong_odd(0)
    fine_smooth(u2, u3, 2, steps - 4, late_rows)
    over_planes(3, steps - 3, last_residual)
    h_wait(OLD_E2)
    x_inner(4)
    over_rows(*late_rows, lambda r: put(u2, 0, r, at(u1, 0, r) + at(e2, 0, r)))
    prolong_even(0)
    fine_smooth(u2, u3, 0, 2, late_rows)
    over_planes(1, 3, last_residual)
    last_residual(0)
    x_edges(5)
    x_inner(5)

    def add_before(r):
        part = pl.ds(r - TOP, CHUNK)
        res[0, :, part, :] = res[0, :, part, :] + at(u3, 0, r)

    over_rows(TOP, end, add_before)

    @pl.when(~last)
    def _():
        rows_wait(xs, rows * len(x_plan))

    for device, jobs in relays.items():

        @pl.when(tm == device)
        def _():
            for slot, _ in jobs:
                rows_wait(fs.at[slot], sum(AROUND))

    h_count(hs, sum(h_rows(group) for group in h_plan))


def store_kernel(steps, rows, blocks, u3, res, field_out, res_out, sem):
    some = steps // 4
    for low in range(0, steps, some):
        for k in range(blocks):
            cols = pl.ds(k * LANES, LANES)
            own = u3.at[pl.ds(1 + low, some), k, pl.ds(TOP, rows), :]
            out = res.at[pl.ds(low, some), k, :, :]
            pltpu.make_async_copy(own, field_out.at[pl.ds(low, some), :, cols], sem.at[0]).start()
            pltpu.make_async_copy(out, res_out.at[pl.ds(low, some), :, cols], sem.at[1]).start()
    pltpu.make_async_copy(field_out, field_out, sem.at[0]).wait()
    pltpu.make_async_copy(res_out, res_out, sem.at[1]).wait()


def shards(source, guess, start_state, conduct):
    steps, rows, cols = source.shape
    blocks = cols // LANES
    half = steps // 2
    tall = rows + 2 * TOP
    f32 = jnp.float32
    hbm = pl.BlockSpec(memory_space=pltpu.HBM)
    vmem = pl.BlockSpec(memory_space=pltpu.VMEM)

    def planes(n):
        return pltpu.VMEM((n, blocks, tall, LANES), f32)

    u3, res = pl.pallas_call(
        functools.partial(cycle_kernel, steps, rows, blocks),
        out_shape=(
            jax.ShapeDtypeStruct((steps + 1, blocks, tall, LANES), f32),
            jax.ShapeDtypeStruct((steps, blocks, rows, LANES), f32),
        ),
        in_specs=[hbm] * 4,
        out_specs=(vmem, vmem),
        scratch_shapes=[
            planes(steps),
            planes(steps + 1),
            planes(steps + 1),
            planes(steps + 1),
            planes(half + 1),
            planes(half + 1),
            planes(half + 1),
            planes(half),
            planes(steps),
            planes(5),
            planes(2),
            pltpu.VMEM((2, 6, blocks, max(AROUND), LANES), f32),
            pltpu.SemaphoreType.DMA((7,)),
            pltpu.SemaphoreType.DMA,
            pltpu.SemaphoreType.DMA((6, 2)),
            pltpu.SemaphoreType.DMA((2, 6)),
            pltpu.SemaphoreType.DMA((2,)),
            pltpu.SemaphoreType.REGULAR,
            pltpu.SemaphoreType.DMA,
            pltpu.SemaphoreType.DMA((9,)),
        ],
        compiler_params=pltpu.CompilerParams(
            collective_id=0, has_side_effects=True, vmem_limit_bytes=44 * 1024 * 1024
        ),
        name="cycle",
    )(*(pltpu.with_memory_space_constraint(a, pltpu.HBM) for a in (source, guess, start_state, conduct)))
    return pl.pallas_call(
        functools.partial(store_kernel, steps, rows, blocks),
        out_shape=(jax.ShapeDtypeStruct(source.shape, f32), jax.ShapeDtypeStruct(source.shape, f32)),
        in_specs=[vmem, vmem],
        out_specs=(hbm, hbm),
        scratch_shapes=[pltpu.SemaphoreType.DMA((2,))],
        compiler_params=pltpu.CompilerParams(vmem_limit_bytes=16 * 1024 * 1024),
        name="store",
    )(u3, res)


def solution(mesh):
    return jax.shard_map(
        shards,
        mesh=mesh,
        in_specs=(
            P("tm", "space", None),
            P("tm", "space", None),
            P("space", None),
            P("space", None),
        ),
        out_specs=(P("tm", "space", None), P("tm", "space", None)),
        check_vma=False,
    )
```

```python
import functools

import jax
import jax.numpy as jnp
from jax import lax
from jax.experimental import pallas as pl
from jax.experimental.pallas import tpu as pltpu
from jax.sharding import PartitionSpec as P

damping = 0.8
MESH = pl.DeviceIdType.MESH
LANES = 128
HALO = 12
TOP = 16
CHUNK = 8
EDGE = (12, 12, 8, 8, 8, 8)
AROUND = (8, 20, 8, 12, 16, 12)


def cycle_kernel(
    steps,
    rows,
    blocks,
    source_hbm,
    guess_hbm,
    start_hbm,
    cond_hbm,
    u3,
    res,
    src,
    gue,
    u1,
    u2,
    e0,
    e1,
    e2,
    rhs,
    tmp,
    coef,
    sums,
    relay,
    load_sem,
    xs,
    xr,
    lr,
    fs,
    meet,
    hs,
    hr,
):
    half = steps // 2
    end = TOP + rows
    tm, sp = lax.axis_index("tm"), lax.axis_index("space")
    n_tm, n_sp = lax.axis_size("tm"), lax.axis_size("space")
    first, last = tm == 0, tm == n_tm - 1
    top, bottom = sp == 0, sp == n_sp - 1
    COND, INV, W, INVK, WK = range(5)

    barrier = pltpu.get_barrier_semaphore()

    def greet(cond, axis, index):
        @pl.when(cond)
        def _():
            pl.semaphore_signal(barrier, inc=1, device_id={axis: index}, device_id_type=MESH)

    greet(~first, "tm", tm - 1)
    greet(~last, "tm", tm + 1)
    greet(~top, "space", sp - 1)
    greet(~bottom, "space", sp + 1)

    def rows_wait(sem, count):
        planes = next(n for n in range(1, count + 1) if count % n == 0 and count // n <= end)
        there = gue.at[pl.ds(0, planes), :, pl.ds(0, count // planes), :]
        pltpu.make_async_copy(there, there, sem).wait()

    def load(group, hbm, lead, buf, at, count):
        out = []
        for k in range(blocks):
            cols = pl.ds(k * LANES, LANES)
            view = hbm.at[:, cols] if lead is None else hbm.at[pl.ds(lead, count), :, cols]
            dst = buf.at[at, k, pl.ds(TOP, rows), :] if lead is None else buf.at[pl.ds(at, count), k, pl.ds(TOP, rows), :]
            out.append(pltpu.make_async_copy(view, dst, load_sem.at[group]))
        return out

    def guess_load(group, low, count):
        return load(group, guess_hbm, low, gue, low + 1, count)

    def source_load(group, low, count):
        return load(group, source_hbm, low, src, low, count)

    def load_wait(group):
        rows_wait(load_sem.at[group], rows * (2, 2, 4, 4, 5, 1, 1)[group])

    for copies in (
        guess_load(0, steps - 2, 2),
        load(1, cond_hbm, None, coef, COND, 1),
        source_load(1, steps - 1, 1),
        guess_load(2, steps - 4, 2),
        source_load(2, steps - 3, 2),
        guess_load(3, steps - 6, 2),
        source_load(3, steps - 5, 2),
        guess_load(4, 0, 2),
        source_load(4, 0, 3),
    ):
        for c in copies:
            c.start()

    @pl.when(first)
    def _():
        for i, buf in enumerate((gue, u3)):
            for c in load(5 + i, start_hbm, None, buf, 0, 1):
                c.start()

    one = jnp.int32(1)
    zero = jnp.int32(0)
    peers = [jnp.where(edge, zero, one) for edge in (first, last, top, bottom)]
    pl.semaphore_wait(barrier, peers[0] + peers[1] + peers[2] + peers[3])

    x_plan = [(gue, steps), (sums, 1), (e0, half), (e1, half), (e2, half), (u3, steps)]
    ways = {0: (3, 0), 1: (3, 1), 2: (1, 0)}
    relays = {3: ((0, 1), (1, 2)), 1: ((0, 3),)}
    FIRST_ROWS, LAST_ROWS, INNER, AROUND_ROWS = range(4)

    def part(i, piece):
        edge, inner = EDGE[i], rows - 2 * EDGE[i] - AROUND[i]
        return pl.ds(
            *((TOP, edge), (end - edge, edge), (TOP + edge, inner), (TOP + edge + inner, AROUND[i]))[piece]
        )

    def x_copy(i, piece):
        buf, plane = x_plan[i]
        return pltpu.make_async_remote_copy(
            src_ref=buf.at[plane, :, part(i, piece), :],
            dst_ref=buf.at[0, :, part(i, piece), :],
            send_sem=xs,
            recv_sem=xr.at[i, piece // 2],
            device_id={"tm": tm + 1},
            device_id_type=MESH,
        )

    def to_relay(i, device, slot):
        buf, plane = x_plan[i]
        return pltpu.make_async_remote_copy(
            src_ref=buf.at[plane, :, part(i, AROUND_ROWS), :],
            dst_ref=relay.at[slot, i, :, pl.ds(0, AROUND[i]), :],
            send_sem=xs,
            recv_sem=lr.at[slot, i],
            device_id={"tm": device},
            device_id_type=MESH,
        )

    def from_relay(i, slot, device):
        return pltpu.make_async_remote_copy(
            src_ref=relay.at[slot, i, :, pl.ds(0, AROUND[i]), :],
            dst_ref=x_plan[i][0].at[0, :, part(i, AROUND_ROWS), :],
            send_sem=fs.at[slot],
            recv_sem=xr.at[i, 1],
            device_id={"tm": device},
            device_id_type=MESH,
        )

    def x_send_edges(i):
        @pl.when(~last)
        def _():
            x_copy(i, FIRST_ROWS).start()
            x_copy(i, LAST_ROWS).start()

    def x_send_around(i):
        for sender, way in ways.items():

            @pl.when(tm == sender)
            def _():
                to_relay(i, *way).start()

    def x_send_inner(*which):
        @pl.when(~last)
        def _():
            for i in which:
                x_copy(i, INNER).start()

    def x_tell(device):
        @pl.when(tm == device)
        def _():
            pl.semaphore_signal(meet, inc=1, device_id={"tm": device - 1}, device_id_type=MESH)

    def x_hear(device):
        @pl.when(tm == device)
        def _():
            pl.semaphore_wait(meet, 1)

    def x_send(i):
        x_send_edges(i)
        x_send_around(i)
        x_send_inner(i)

    def x_relay(i):
        for device, jobs in relays.items():

            @pl.when(tm == device)
            def _():
                for slot, final in jobs:
                    to_relay(i, device, slot).wait_recv()
                    from_relay(i, slot, final).start()

    def x_edges(i):
        @pl.when(~first)
        def _():
            rows_wait(xr.at[i, 0], 2 * EDGE[i])

        if i in (0, 5):

            @pl.when(first)
            def _():
                load_wait(5 if i == 0 else 6)

    def x_inner(i):
        @pl.when(~first)
        def _():
            rows_wait(xr.at[i, 1], rows - 2 * EDGE[i])

    h_plan = [
        ((gue, steps - 1, 2, 11), (coef, COND, 1, 10), (src, steps - 1, 1, 10)),
        ((gue, steps - 3, 2, 11), (src, steps - 3, 2, 10)),
        ((gue, steps - 5, 2, 11), (src, steps - 5, 2, 10)),
        ((gue, 1, 2, 11), (src, 0, 3, 10)),
        ((gue, 0, 1, 10),),
        ((sums, 0, 1, 9),),
        ((e0, 0, 1, 6),),
        ((e1, 0, 1, 4),),
        ((e2, 0, 1, 3),),
    ]
    OLD_GUESS, OLD_SUM, OLD_E0, OLD_E1, OLD_E2 = range(4, 9)

    def down_copy(i, buf, plane, count, width):
        return pltpu.make_async_remote_copy(
            src_ref=buf.at[pl.ds(plane, count), :, pl.ds(end - width, width), :],
            dst_ref=buf.at[pl.ds(plane, count), :, pl.ds(TOP - width, width), :],
            send_sem=hs,
            recv_sem=hr.at[i],
            device_id={"space": sp + 1},
            device_id_type=MESH,
        )

    def up_copy(i, buf, plane, count, width):
        return pltpu.make_async_remote_copy(
            src_ref=buf.at[pl.ds(plane, count), :, pl.ds(TOP, width), :],
            dst_ref=buf.at[pl.ds(plane, count), :, pl.ds(end, width), :],
            send_sem=hs,
            recv_sem=hr.at[i],
            device_id={"space": sp - 1},
            device_id_type=MESH,
        )

    def h_send(i, low=0, high=9):
        @pl.when(~bottom)
        def _():
            for item in h_plan[i][low:high]:
                down_copy(i, *item).start()

        @pl.when(~top)
        def _():
            for item in h_plan[i][low:high]:
                up_copy(i, *item).start()

    def h_rows(group):
        return sum(count * width for _, _, count, width in group)

    def h_count(sem, count):
        @pl.when(top | bottom)
        def _():
            rows_wait(sem, count)

        @pl.when(~top & ~bottom)
        def _():
            rows_wait(sem, 2 * count)

    def h_wait(i):
        h_count(hr.at[i], h_rows(h_plan[i]))

    def at(buf, n, r):
        return buf[n, :, pl.ds(r, CHUNK), :]

    def put(buf, n, r, value):
        buf[n, :, pl.ds(r, CHUNK), :] = value

    def sideways(v):
        lane = lax.broadcasted_iota(jnp.int32, v.shape, 2)
        edge = jnp.zeros((1,) + v.shape[1:], jnp.float32)
        fwd = pltpu.roll(v, 1, 2)
        bwd = pltpu.roll(v, LANES - 1, 2)
        left = jnp.where(lane == 0, jnp.concatenate([edge, fwd[:-1]], axis=0), fwd)
        right = jnp.where(lane == LANES - 1, jnp.concatenate([bwd[1:], edge], axis=0), bwd)
        return left + right

    def with_sum(buf, n, r):
        v = at(buf, n, r)
        return v, (at(buf, n, r - 1) + at(buf, n, r + 1)) + sideways(v)

    def over_rows(low, high, body):
        count = (high - low) // CHUNK

        def step(i, carry):
            body(low + i * CHUNK)
            return carry

        lax.fori_loop(0, count, step, 0, unroll=True)

    def over_planes(low, high, body):
        if high - low == 1:
            body(low)
        else:

            def step(i, carry):
                body(i)
                return carry

            lax.fori_loop(low, high, step, 0)

    def grown(extra):
        return (TOP - extra, end + extra)

    fine_rows, coarse_rows, late_rows = grown(12), grown(8), grown(4)

    def fine_smooth(frm, to, low, high, where):
        def first_pass(n):
            def chunk(r):
                v, s = with_sum(frm, n + 1, r)
                rest = at(src, n, r) + at(frm, n, r)
                put(tmp, n, r, damping * (at(coef, INV, r) * rest + at(coef, W, r) * s - v))

            over_rows(*where, chunk)

        def second_pass(n):
            def chunk(r):
                v, s = with_sum(tmp, n, r)
                put(to, n + 1, r, at(frm, n + 1, r) + (v + at(coef, W, r) * s))

            over_rows(*where, chunk)

        over_planes(low, high, first_pass)
        over_planes(low, high, second_pass)

    def smooth_before():
        def first_pass(r):
            v, s = with_sum(gue, 0, r)
            put(tmp, 0, r, damping * (at(coef, INV, r) * at(sums, 0, r) + at(coef, W, r) * s - v))

        def second_pass(r):
            v, s = with_sum(tmp, 0, r)
            put(u1, 0, r, at(gue, 0, r) + (v + at(coef, W, r) * s))

        @pl.when(first)
        def _():
            over_rows(*fine_rows, lambda r: put(u1, 0, r, at(gue, 0, r)))

        @pl.when(~first)
        def _():
            over_rows(*fine_rows, first_pass)
            over_rows(*fine_rows, second_pass)

    def restrict(m):
        def chunk(r):
            a, sa = at(u1, 2 * m + 1, r), at(u1, 2 * m + 1, r - 1) + at(u1, 2 * m + 1, r + 1)
            b, sb = at(u1, 2 * m + 2, r), at(u1, 2 * m + 2, r - 1) + at(u1, 2 * m + 2, r + 1)
            pair = a + b
            around = (sa + sb) + sideways(pair)
            total = at(src, 2 * m, r) + at(src, 2 * m + 1, r) + (at(u1, 2 * m, r) - b)
            total = total - at(coef, COND, r) * (4.0 * pair - around)
            put(rhs, m, r, at(coef, INVK, r) * total)

        over_rows(*coarse_rows, chunk)

    def coarse_first(m):
        def chunk(r):
            v, s = with_sum(rhs, m, r)
            put(e0, m + 1, r, damping * (v + at(coef, WK, r) * s))

        over_rows(*coarse_rows, chunk)

    def coarse_sweep(frm, to, m, slot):
        def first_pass(r):
            v, s = with_sum(frm, m + 1, r)
            rest = at(rhs, m, r) + at(coef, INVK, r) * at(frm, m, r)
            put(tmp, slot, r, damping * (rest + at(coef, WK, r) * s - v))

        def second_pass(r):
            v, s = with_sum(tmp, slot, r)
            put(to, m + 1, r, at(frm, m + 1, r) + (v + at(coef, WK, r) * s))

        where = late_rows if to is e2 else coarse_rows
        over_rows(*where, first_pass)
        over_rows(*where, second_pass)

    def prolong_odd(m):
        over_rows(*late_rows, lambda r: put(u2, 2 * m + 2, r, at(u1, 2 * m + 2, r) + at(e2, m + 1, r)))

    def prolong_even(m):
        over_rows(
            *late_rows,
            lambda r: put(u2, 2 * m + 1, r, at(u1, 2 * m + 1, r) + 0.5 * (at(e2, m, r) + at(e2, m + 1, r))),
        )

    def last_residual(n):
        def chunk(r):
            v, s = with_sum(u3, n + 1, r)
            rest = at(src, n, r) - v if isinstance(n, int) and n == 0 else at(src, n, r) + (at(u3, n, r) - v)
            res[n, :, pl.ds(r - TOP, CHUNK), :] = rest - at(coef, COND, r) * (4.0 * v - s)

        over_rows(TOP, end, chunk)

    def clear(low):
        zeros = jnp.zeros((blocks, HALO, LANES), jnp.float32)

        def planes(buf, a, b):
            for n in range(a, b):
                buf[n, :, pl.ds(low, HALO), :] = zeros

        planes(gue, 0, steps + 1)
        planes(src, 0, steps)
        planes(coef, COND, COND + 1)
        for buf in (sums, e0, e1, e2):
            planes(buf, 0, 1)

    @pl.when(top)
    def _():
        clear(TOP - HALO)

    @pl.when(bottom)
    def _():
        clear(end)

    @pl.when(first)
    def _():
        for buf in (sums, e0, e1, e2):
            buf[0, :, pl.ds(TOP, rows), :] = jnp.zeros((blocks, rows, LANES), jnp.float32)

    odd = lax.rem(sp, 2) == 1

    def x_send_inner_if(turn, *which):
        @pl.when(turn & ~last)
        def _():
            for i in which:
                x_copy(i, INNER).start()

    x_tell(2)
    load_wait(0)
    x_send_edges(0)
    x_send_inner(0)
    h_send(0, 0, 1)
    load_wait(1)
    over_rows(TOP, end, lambda r: put(sums, 1, r, at(src, steps - 1, r) + at(gue, steps - 1, r)))
    h_send(0, 1)
    x_send_edges(1)
    x_send_inner(1)
    x_hear(1)
    x_tell(1)
    load_wait(2)
    h_send(1)
    load_wait(3)
    h_send(2)
    load_wait(4)
    h_send(3)
    x_hear(0)
    x_send_around(1)
    x_send_around(0)

    def coefficients(r):
        c = at(coef, COND, r)
        inv = 1.0 / (1.0 + 4.0 * c)
        invk = 1.0 / (1.0 + 8.0 * c)
        put(coef, INV, r, inv)
        put(coef, W, r, c * inv)
        put(coef, INVK, r, invk)
        put(coef, WK, r, (2.0 * c) * invk)

    h_wait(0)
    over_rows(*fine_rows, coefficients)
    fine_smooth(gue, u1, steps - 1, steps, fine_rows)
    h_wait(1)
    fine_smooth(gue, u1, steps - 3, steps - 1, fine_rows)
    x_relay(1)
    restrict(half - 1)
    coarse_first(half - 1)
    x_send(2)
    x_edges(0)
    h_send(OLD_GUESS)
    x_relay(0)
    h_wait(2)
    fine_smooth(gue, u1, steps - 5, steps - 3, fine_rows)
    restrict(half - 2)
    coarse_first(half - 2)
    coarse_sweep(e0, e1, half - 1, 0)
    x_send_edges(3)
    x_send_around(3)
    x_edges(1)
    h_send(OLD_SUM)
    h_wait(3)
    fine_smooth(gue, u1, 1, steps - 5, fine_rows)
    restrict(half - 3)
    coarse_first(half - 3)
    coarse_sweep(e0, e1, half - 2, 1)
    coarse_sweep(e1, e2, half - 1, 2)
    x_send_edges(4)
    x_send_around(4)
    x_send_inner_if(~odd, 3, 4)
    x_edges(2)
    h_send(OLD_E0)
    h_wait(OLD_GUESS)
    x_inner(0)
    fine_smooth(gue, u1, 0, 1, fine_rows)
    x_relay(2)

    h_wait(OLD_SUM)
    x_inner(1)
    smooth_before()
    restrict(0)
    coarse_first(0)
    x_send_inner_if(odd, 3, 4)
    coarse_sweep(e0, e1, 1, 3)
    coarse_sweep(e1, e2, 2, 4)
    x_edges(3)
    h_send(OLD_E1)
    x_relay(3)
    prolong_odd(half - 1)
    prolong_even(half - 1)
    fine_smooth(u2, u3, steps - 1, steps, late_rows)
    x_send(5)
    x_edges(4)
    h_send(OLD_E2)
    prolong_odd(half - 2)
    fine_smooth(u2, u3, steps - 2, steps - 1, late_rows)
    last_residual(steps - 1)
    h_wait(OLD_E0)
    x_inner(2)
    coarse_sweep(e0, e1, 0, 5)
    coarse_sweep(e1, e2, 1, 6)
    x_relay(4)
    prolong_even(half - 2)
    prolong_odd(half - 3)
    fine_smooth(u2, u3, steps - 4, steps - 2, late_rows)
    h_wait(OLD_E1)
    x_inner(3)
    coarse_sweep(e1, e2, 0, 7)
    over_planes(steps - 3, steps - 1, last_residual)
    x_relay(5)
    prolong_even(1)
    prolong_odd(0)
    fine_smooth(u2, u3, 2, steps - 4, late_rows)
    over_planes(3, steps - 3, last_residual)
    h_wait(OLD_E2)
    x_inner(4)
    over_rows(*late_rows, lambda r: put(u2, 0, r, at(u1, 0, r) + at(e2, 0, r)))
    prolong_even(0)
    fine_smooth(u2, u3, 0, 2, late_rows)
    over_planes(1, 3, last_residual)
    last_residual(0)
    x_edges(5)
    x_inner(5)

    def add_before(r):
        part = pl.ds(r - TOP, CHUNK)
        res[0, :, part, :] = res[0, :, part, :] + at(u3, 0, r)

    over_rows(TOP, end, add_before)

    @pl.when(~last)
    def _():
        rows_wait(xs, rows * len(x_plan))

    for device, jobs in relays.items():

        @pl.when(tm == device)
        def _():
            for slot, _ in jobs:
                rows_wait(fs.at[slot], sum(AROUND))

    h_count(hs, sum(h_rows(group) for group in h_plan))


def store_kernel(steps, rows, blocks, u3, res, field_out, res_out, sem):
    some = steps // 4
    for low in range(0, steps, some):
        for k in range(blocks):
            cols = pl.ds(k * LANES, LANES)
            own = u3.at[pl.ds(1 + low, some), k, pl.ds(TOP, rows), :]
            out = res.at[pl.ds(low, some), k, :, :]
            pltpu.make_async_copy(own, field_out.at[pl.ds(low, some), :, cols], sem.at[0]).start()
            pltpu.make_async_copy(out, res_out.at[pl.ds(low, some), :, cols], sem.at[1]).start()
    pltpu.make_async_copy(field_out, field_out, sem.at[0]).wait()
    pltpu.make_async_copy(res_out, res_out, sem.at[1]).wait()


def shards(source, guess, start_state, conduct):
    steps, rows, cols = source.shape
    blocks = cols // LANES
    half = steps // 2
    tall = rows + 2 * TOP
    f32 = jnp.float32
    hbm = pl.BlockSpec(memory_space=pltpu.HBM)
    vmem = pl.BlockSpec(memory_space=pltpu.VMEM)

    def planes(n):
        return pltpu.VMEM((n, blocks, tall, LANES), f32)

    u3, res = pl.pallas_call(
        functools.partial(cycle_kernel, steps, rows, blocks),
        out_shape=(
            jax.ShapeDtypeStruct((steps + 1, blocks, tall, LANES), f32),
            jax.ShapeDtypeStruct((steps, blocks, rows, LANES), f32),
        ),
        in_specs=[hbm] * 4,
        out_specs=(vmem, vmem),
        scratch_shapes=[
            planes(steps),
            planes(steps + 1),
            planes(steps + 1),
            planes(steps + 1),
            planes(half + 1),
            planes(half + 1),
            planes(half + 1),
            planes(half),
            planes(steps),
            planes(5),
            planes(2),
            pltpu.VMEM((2, 6, blocks, max(AROUND), LANES), f32),
            pltpu.SemaphoreType.DMA((7,)),
            pltpu.SemaphoreType.DMA,
            pltpu.SemaphoreType.DMA((6, 2)),
            pltpu.SemaphoreType.DMA((2, 6)),
            pltpu.SemaphoreType.DMA((2,)),
            pltpu.SemaphoreType.REGULAR,
            pltpu.SemaphoreType.DMA,
            pltpu.SemaphoreType.DMA((9,)),
        ],
        compiler_params=pltpu.CompilerParams(
            collective_id=0, has_side_effects=True, vmem_limit_bytes=44 * 1024 * 1024
        ),
        name="cycle",
    )(*(pltpu.with_memory_space_constraint(a, pltpu.HBM) for a in (source, guess, start_state, conduct)))
    return pl.pallas_call(
        functools.partial(store_kernel, steps, rows, blocks),
        out_shape=(jax.ShapeDtypeStruct(source.shape, f32), jax.ShapeDtypeStruct(source.shape, f32)),
        in_specs=[vmem, vmem],
        out_specs=(hbm, hbm),
        scratch_shapes=[pltpu.SemaphoreType.DMA((2,))],
        compiler_params=pltpu.CompilerParams(vmem_limit_bytes=16 * 1024 * 1024),
        name="store",
    )(u3, res)


def solution(mesh):
    return jax.shard_map(
        shards,
        mesh=mesh,
        in_specs=(
            P("tm", "space", None),
            P("tm", "space", None),
            P("space", None),
            P("space", None),
        ),
        out_specs=(P("tm", "space", None), P("tm", "space", None)),
        check_vma=False,
    )
```

```python
import functools

import jax
import jax.numpy as jnp
from jax import lax
from jax.experimental import pallas as pl
from jax.experimental.pallas import tpu as pltpu
from jax.sharding import PartitionSpec as P

damping = 0.8
MESH = pl.DeviceIdType.MESH
LANES = 128
HALO = 12
TOP = 16
CHUNK = 8
EDGE = (12, 12, 8, 8, 8, 8)
AROUND = (8, 20, 8, 12, 16, 12)


def cycle_kernel(
    steps,
    rows,
    blocks,
    source_hbm,
    guess_hbm,
    start_hbm,
    cond_hbm,
    u3,
    res,
    src,
    gue,
    u1,
    u2,
    e0,
    e1,
    e2,
    rhs,
    tmp,
    coef,
    sums,
    relay,
    load_sem,
    xs,
    xr,
    lr,
    fs,
    meet,
    hs,
    hr,
):
    half = steps // 2
    end = TOP + rows
    tm, sp = lax.axis_index("tm"), lax.axis_index("space")
    n_tm, n_sp = lax.axis_size("tm"), lax.axis_size("space")
    first, last = tm == 0, tm == n_tm - 1
    top, bottom = sp == 0, sp == n_sp - 1
    COND, INV, W, INVK, WK = range(5)

    barrier = pltpu.get_barrier_semaphore()

    def greet(cond, axis, index):
        @pl.when(cond)
        def _():
            pl.semaphore_signal(barrier, inc=1, device_id={axis: index}, device_id_type=MESH)

    greet(~first, "tm", tm - 1)
    greet(~last, "tm", tm + 1)
    greet(~top, "space", sp - 1)
    greet(~bottom, "space", sp + 1)

    def rows_wait(sem, count):
        planes = next(n for n in range(1, count + 1) if count % n == 0 and count // n <= end)
        there = gue.at[pl.ds(0, planes), :, pl.ds(0, count // planes), :]
        pltpu.make_async_copy(there, there, sem).wait()

    def load(group, hbm, lead, buf, at, count):
        out = []
        for k in range(blocks):
            cols = pl.ds(k * LANES, LANES)
            view = hbm.at[:, cols] if lead is None else hbm.at[pl.ds(lead, count), :, cols]
            dst = buf.at[at, k, pl.ds(TOP, rows), :] if lead is None else buf.at[pl.ds(at, count), k, pl.ds(TOP, rows), :]
            out.append(pltpu.make_async_copy(view, dst, load_sem.at[group]))
        return out

    def guess_load(group, low, count):
        return load(group, guess_hbm, low, gue, low + 1, count)

    def source_load(group, low, count):
        return load(group, source_hbm, low, src, low, count)

    def load_wait(group):
        rows_wait(load_sem.at[group], rows * (2, 2, 4, 4, 5, 1, 1)[group])

    for copies in (
        guess_load(0, steps - 2, 2),
        load(1, cond_hbm, None, coef, COND, 1),
        source_load(1, steps - 1, 1),
        guess_load(2, steps - 4, 2),
        source_load(2, steps - 3, 2),
        guess_load(3, steps - 6, 2),
        source_load(3, steps - 5, 2),
        guess_load(4, 0, 2),
        source_load(4, 0, 3),
    ):
        for c in copies:
            c.start()

    @pl.when(first)
    def _():
        for i, buf in enumerate((gue, u3)):
            for c in load(5 + i, start_hbm, None, buf, 0, 1):
                c.start()

    one = jnp.int32(1)
    zero = jnp.int32(0)
    peers = [jnp.where(edge, zero, one) for edge in (first, last, top, bottom)]
    pl.semaphore_wait(barrier, peers[0] + peers[1] + peers[2] + peers[3])

    x_plan = [(gue, steps), (sums, 1), (e0, half), (e1, half), (e2, half), (u3, steps)]
    ways = {0: (3, 0), 1: (3, 1), 2: (1, 0)}
    relays = {3: ((0, 1), (1, 2)), 1: ((0, 3),)}
    FIRST_ROWS, LAST_ROWS, INNER, AROUND_ROWS = range(4)

    def part(i, piece):
        edge, inner = EDGE[i], rows - 2 * EDGE[i] - AROUND[i]
        return pl.ds(
            *((TOP, edge), (end - edge, edge), (TOP + edge, inner), (TOP + edge + inner, AROUND[i]))[piece]
        )

    def x_copy(i, piece):
        buf, plane = x_plan[i]
        return pltpu.make_async_remote_copy(
            src_ref=buf.at[plane, :, part(i, piece), :],
            dst_ref=buf.at[0, :, part(i, piece), :],
            send_sem=xs,
            recv_sem=xr.at[i, piece // 2],
            device_id={"tm": tm + 1},
            device_id_type=MESH,
        )

    def to_relay(i, device, slot):
        buf, plane = x_plan[i]
        return pltpu.make_async_remote_copy(
            src_ref=buf.at[plane, :, part(i, AROUND_ROWS), :],
            dst_ref=relay.at[slot, i, :, pl.ds(0, AROUND[i]), :],
            send_sem=xs,
            recv_sem=lr.at[slot, i],
            device_id={"tm": device},
            device_id_type=MESH,
        )

    def from_relay(i, slot, device):
        return pltpu.make_async_remote_copy(
            src_ref=relay.at[slot, i, :, pl.ds(0, AROUND[i]), :],
            dst_ref=x_plan[i][0].at[0, :, part(i, AROUND_ROWS), :],
            send_sem=fs.at[slot],
            recv_sem=xr.at[i, 1],
            device_id={"tm": device},
            device_id_type=MESH,
        )

    def x_send_edges(i):
        @pl.when(~last)
        def _():
            x_copy(i, FIRST_ROWS).start()
            x_copy(i, LAST_ROWS).start()

    def x_send_around(i):
        for sender, way in ways.items():

            @pl.when(tm == sender)
            def _():
                to_relay(i, *way).start()

    def x_send_inner(*which):
        @pl.when(~last)
        def _():
            for i in which:
                x_copy(i, INNER).start()

    def x_tell(device):
        @pl.when(tm == device)
        def _():
            pl.semaphore_signal(meet, inc=1, device_id={"tm": device - 1}, device_id_type=MESH)

    def x_hear(device):
        @pl.when(tm == device)
        def _():
            pl.semaphore_wait(meet, 1)

    def x_send(i):
        x_send_edges(i)
        x_send_around(i)
        x_send_inner(i)

    def x_relay(i):
        for device, jobs in relays.items():

            @pl.when(tm == device)
            def _():
                for slot, final in jobs:
                    to_relay(i, device, slot).wait_recv()
                    from_relay(i, slot, final).start()

    def x_edges(i):
        @pl.when(~first)
        def _():
            rows_wait(xr.at[i, 0], 2 * EDGE[i])

        if i in (0, 5):

            @pl.when(first)
            def _():
                load_wait(5 if i == 0 else 6)

    def x_inner(i):
        @pl.when(~first)
        def _():
            rows_wait(xr.at[i, 1], rows - 2 * EDGE[i])

    h_plan = [
        ((gue, steps - 1, 2, 11), (coef, COND, 1, 10), (src, steps - 1, 1, 10)),
        ((gue, steps - 3, 2, 11), (src, steps - 3, 2, 10)),
        ((gue, steps - 5, 2, 11), (src, steps - 5, 2, 10)),
        ((gue, 1, 2, 11), (src, 0, 3, 10)),
        ((gue, 0, 1, 10),),
        ((sums, 0, 1, 9),),
        ((e0, 0, 1, 6),),
        ((e1, 0, 1, 4),),
        ((e2, 0, 1, 3),),
    ]
    OLD_GUESS, OLD_SUM, OLD_E0, OLD_E1, OLD_E2 = range(4, 9)

    def down_copy(i, buf, plane, count, width):
        return pltpu.make_async_remote_copy(
            src_ref=buf.at[pl.ds(plane, count), :, pl.ds(end - width, width), :],
            dst_ref=buf.at[pl.ds(plane, count), :, pl.ds(TOP - width, width), :],
            send_sem=hs,
            recv_sem=hr.at[i],
            device_id={"space": sp + 1},
            device_id_type=MESH,
        )

    def up_copy(i, buf, plane, count, width):
        return pltpu.make_async_remote_copy(
            src_ref=buf.at[pl.ds(plane, count), :, pl.ds(TOP, width), :],
            dst_ref=buf.at[pl.ds(plane, count), :, pl.ds(end, width), :],
            send_sem=hs,
            recv_sem=hr.at[i],
            device_id={"space": sp - 1},
            device_id_type=MESH,
        )

    def h_send(i, low=0, high=9):
        @pl.when(~bottom)
        def _():
            for item in h_plan[i][low:high]:
                down_copy(i, *item).start()

        @pl.when(~top)
        def _():
            for item in h_plan[i][low:high]:
                up_copy(i, *item).start()

    def h_rows(group):
        return sum(count * width for _, _, count, width in group)

    def h_count(sem, count):
        @pl.when(top | bottom)
        def _():
            rows_wait(sem, count)

        @pl.when(~top & ~bottom)
        def _():
            rows_wait(sem, 2 * count)

    def h_wait(i):
        h_count(hr.at[i], h_rows(h_plan[i]))

    def at(buf, n, r):
        return buf[n, :, pl.ds(r, CHUNK), :]

    def put(buf, n, r, value):
        buf[n, :, pl.ds(r, CHUNK), :] = value

    def sideways(v):
        lane = lax.broadcasted_iota(jnp.int32, v.shape, 2)
        edge = jnp.zeros((1,) + v.shape[1:], jnp.float32)
        fwd = pltpu.roll(v, 1, 2)
        bwd = pltpu.roll(v, LANES - 1, 2)
        left = jnp.where(lane == 0, jnp.concatenate([edge, fwd[:-1]], axis=0), fwd)
        right = jnp.where(lane == LANES - 1, jnp.concatenate([bwd[1:], edge], axis=0), bwd)
        return left + right

    def with_sum(buf, n, r):
        v = at(buf, n, r)
        return v, (at(buf, n, r - 1) + at(buf, n, r + 1)) + sideways(v)

    def over_rows(low, high, body):
        count = (high - low) // CHUNK

        def step(i, carry):
            body(low + i * CHUNK)
            return carry

        lax.fori_loop(0, count, step, 0, unroll=True)

    def over_planes(low, high, body):
        if high - low == 1:
            body(low)
        else:

            def step(i, carry):
                body(i)
                return carry

            lax.fori_loop(low, high, step, 0)

    def grown(extra):
        return (TOP - extra, end + extra)

    fine_rows, coarse_rows, late_rows = grown(12), grown(8), grown(4)

    def fine_smooth(frm, to, low, high, where):
        def first_pass(n):
            def chunk(r):
                v, s = with_sum(frm, n + 1, r)
                rest = at(src, n, r) + at(frm, n, r)
                put(tmp, n, r, damping * (at(coef, INV, r) * rest + at(coef, W, r) * s - v))

            over_rows(*where, chunk)

        def second_pass(n):
            def chunk(r):
                v, s = with_sum(tmp, n, r)
                put(to, n + 1, r, at(frm, n + 1, r) + (v + at(coef, W, r) * s))

            over_rows(*where, chunk)

        over_planes(low, high, first_pass)
        over_planes(low, high, second_pass)

    def smooth_before():
        def first_pass(r):
            v, s = with_sum(gue, 0, r)
            put(tmp, 0, r, damping * (at(coef, INV, r) * at(sums, 0, r) + at(coef, W, r) * s - v))

        def second_pass(r):
            v, s = with_sum(tmp, 0, r)
            put(u1, 0, r, at(gue, 0, r) + (v + at(coef, W, r) * s))

        @pl.when(first)
        def _():
            over_rows(*fine_rows, lambda r: put(u1, 0, r, at(gue, 0, r)))

        @pl.when(~first)
        def _():
            over_rows(*fine_rows, first_pass)
            over_rows(*fine_rows, second_pass)

    def restrict(m):
        def chunk(r):
            a, sa = at(u1, 2 * m + 1, r), at(u1, 2 * m + 1, r - 1) + at(u1, 2 * m + 1, r + 1)
            b, sb = at(u1, 2 * m + 2, r), at(u1, 2 * m + 2, r - 1) + at(u1, 2 * m + 2, r + 1)
            pair = a + b
            around = (sa + sb) + sideways(pair)
            total = at(src, 2 * m, r) + at(src, 2 * m + 1, r) + (at(u1, 2 * m, r) - b)
            total = total - at(coef, COND, r) * (4.0 * pair - around)
            put(rhs, m, r, at(coef, INVK, r) * total)

        over_rows(*coarse_rows, chunk)

    def coarse_first(m):
        def chunk(r):
            v, s = with_sum(rhs, m, r)
            put(e0, m + 1, r, damping * (v + at(coef, WK, r) * s))

        over_rows(*coarse_rows, chunk)

    def coarse_sweep(frm, to, m, slot):
        def first_pass(r):
            v, s = with_sum(frm, m + 1, r)
            rest = at(rhs, m, r) + at(coef, INVK, r) * at(frm, m, r)
            put(tmp, slot, r, damping * (rest + at(coef, WK, r) * s - v))

        def second_pass(r):
            v, s = with_sum(tmp, slot, r)
            put(to, m + 1, r, at(frm, m + 1, r) + (v + at(coef, WK, r) * s))

        where = late_rows if to is e2 else coarse_rows
        over_rows(*where, first_pass)
        over_rows(*where, second_pass)

    def prolong_odd(m):
        over_rows(*late_rows, lambda r: put(u2, 2 * m + 2, r, at(u1, 2 * m + 2, r) + at(e2, m + 1, r)))

    def prolong_even(m):
        over_rows(
            *late_rows,
            lambda r: put(u2, 2 * m + 1, r, at(u1, 2 * m + 1, r) + 0.5 * (at(e2, m, r) + at(e2, m + 1, r))),
        )

    def last_residual(n):
        def chunk(r):
            v, s = with_sum(u3, n + 1, r)
            rest = at(src, n, r) - v if isinstance(n, int) and n == 0 else at(src, n, r) + (at(u3, n, r) - v)
            res[n, :, pl.ds(r - TOP, CHUNK), :] = rest - at(coef, COND, r) * (4.0 * v - s)

        over_rows(TOP, end, chunk)

    def clear(low):
        zeros = jnp.zeros((blocks, HALO, LANES), jnp.float32)

        def planes(buf, a, b):
            for n in range(a, b):
                buf[n, :, pl.ds(low, HALO), :] = zeros

        planes(gue, 0, steps + 1)
        planes(src, 0, steps)
        planes(coef, COND, COND + 1)
        for buf in (sums, e0, e1, e2):
            planes(buf, 0, 1)

    @pl.when(top)
    def _():
        clear(TOP - HALO)

    @pl.when(bottom)
    def _():
        clear(end)

    @pl.when(first)
    def _():
        for buf in (sums, e0, e1, e2):
            buf[0, :, pl.ds(TOP, rows), :] = jnp.zeros((blocks, rows, LANES), jnp.float32)

    odd = lax.rem(sp, 2) == 1

    def x_send_inner_if(turn, *which):
        @pl.when(turn & ~last)
        def _():
            for i in which:
                x_copy(i, INNER).start()

    x_tell(2)
    load_wait(0)
    x_send_edges(0)
    x_send_inner(0)
    h_send(0, 0, 1)
    load_wait(1)
    over_rows(TOP, end, lambda r: put(sums, 1, r, at(src, steps - 1, r) + at(gue, steps - 1, r)))
    h_send(0, 1)
    x_send_edges(1)
    x_send_inner(1)
    x_hear(1)
    x_tell(1)
    load_wait(2)
    h_send(1)
    load_wait(3)
    h_send(2)
    load_wait(4)
    h_send(3)
    x_hear(0)
    x_send_around(1)
    x_send_around(0)

    def coefficients(r):
        c = at(coef, COND, r)
        inv = 1.0 / (1.0 + 4.0 * c)
        invk = 1.0 / (1.0 + 8.0 * c)
        put(coef, INV, r, inv)
        put(coef, W, r, c * inv)
        put(coef, INVK, r, invk)
        put(coef, WK, r, (2.0 * c) * invk)

    h_wait(0)
    over_rows(*fine_rows, coefficients)
    fine_smooth(gue, u1, steps - 1, steps, fine_rows)
    h_wait(1)
    fine_smooth(gue, u1, steps - 3, steps - 1, fine_rows)
    x_relay(1)
    restrict(half - 1)
    coarse_first(half - 1)
    x_send(2)
    x_edges(0)
    h_send(OLD_GUESS)
    x_relay(0)
    h_wait(2)
    fine_smooth(gue, u1, steps - 5, steps - 3, fine_rows)
    restrict(half - 2)
    coarse_first(half - 2)
    coarse_sweep(e0, e1, half - 1, 0)
    x_send_edges(3)
    x_send_around(3)
    x_edges(1)
    h_send(OLD_SUM)
    h_wait(3)
    fine_smooth(gue, u1, 1, steps - 5, fine_rows)
    restrict(half - 3)
    coarse_first(half - 3)
    coarse_sweep(e0, e1, half - 2, 1)
    coarse_sweep(e1, e2, half - 1, 2)
    x_send_edges(4)
    x_send_around(4)
    x_send_inner_if(~odd, 3, 4)
    x_edges(2)
    h_send(OLD_E0)
    h_wait(OLD_GUESS)
    x_inner(0)
    fine_smooth(gue, u1, 0, 1, fine_rows)
    x_relay(2)

    h_wait(OLD_SUM)
    x_inner(1)
    smooth_before()
    restrict(0)
    coarse_first(0)
    x_send_inner_if(odd, 3, 4)
    coarse_sweep(e0, e1, 1, 3)
    coarse_sweep(e1, e2, 2, 4)
    x_edges(3)
    h_send(OLD_E1)
    x_relay(3)
    prolong_odd(half - 1)
    prolong_even(half - 1)
    fine_smooth(u2, u3, steps - 1, steps, late_rows)
    x_send(5)
    x_edges(4)
    h_send(OLD_E2)
    prolong_odd(half - 2)
    fine_smooth(u2, u3, steps - 2, steps - 1, late_rows)
    last_residual(steps - 1)
    h_wait(OLD_E0)
    x_inner(2)
    coarse_sweep(e0, e1, 0, 5)
    coarse_sweep(e1, e2, 1, 6)
    x_relay(4)
    prolong_even(half - 2)
    prolong_odd(half - 3)
    fine_smooth(u2, u3, steps - 4, steps - 2, late_rows)
    h_wait(OLD_E1)
    x_inner(3)
    coarse_sweep(e1, e2, 0, 7)
    x_relay(5)
    over_planes(steps - 3, steps - 1, last_residual)
    prolong_even(1)
    prolong_odd(0)
    fine_smooth(u2, u3, 2, steps - 4, late_rows)
    over_planes(3, steps - 3, last_residual)
    h_wait(OLD_E2)
    x_inner(4)
    over_rows(*late_rows, lambda r: put(u2, 0, r, at(u1, 0, r) + at(e2, 0, r)))
    prolong_even(0)
    fine_smooth(u2, u3, 0, 2, late_rows)
    over_planes(1, 3, last_residual)
    last_residual(0)
    x_edges(5)
    x_inner(5)

    def add_before(r):
        part = pl.ds(r - TOP, CHUNK)
        res[0, :, part, :] = res[0, :, part, :] + at(u3, 0, r)

    over_rows(TOP, end, add_before)

    @pl.when(~last)
    def _():
        rows_wait(xs, rows * len(x_plan))

    for device, jobs in relays.items():

        @pl.when(tm == device)
        def _():
            for slot, _ in jobs:
                rows_wait(fs.at[slot], sum(AROUND))

    h_count(hs, sum(h_rows(group) for group in h_plan))


def store_kernel(steps, rows, blocks, u3, res, field_out, res_out, sem):
    some = steps // 4
    for low in range(0, steps, some):
        for k in range(blocks):
            cols = pl.ds(k * LANES, LANES)
            own = u3.at[pl.ds(1 + low, some), k, pl.ds(TOP, rows), :]
            out = res.at[pl.ds(low, some), k, :, :]
            pltpu.make_async_copy(own, field_out.at[pl.ds(low, some), :, cols], sem.at[0]).start()
            pltpu.make_async_copy(out, res_out.at[pl.ds(low, some), :, cols], sem.at[1]).start()
    pltpu.make_async_copy(field_out, field_out, sem.at[0]).wait()
    pltpu.make_async_copy(res_out, res_out, sem.at[1]).wait()


def shards(source, guess, start_state, conduct):
    steps, rows, cols = source.shape
    blocks = cols // LANES
    half = steps // 2
    tall = rows + 2 * TOP
    f32 = jnp.float32
    hbm = pl.BlockSpec(memory_space=pltpu.HBM)
    vmem = pl.BlockSpec(memory_space=pltpu.VMEM)

    def planes(n):
        return pltpu.VMEM((n, blocks, tall, LANES), f32)

    u3, res = pl.pallas_call(
        functools.partial(cycle_kernel, steps, rows, blocks),
        out_shape=(
            jax.ShapeDtypeStruct((steps + 1, blocks, tall, LANES), f32),
            jax.ShapeDtypeStruct((steps, blocks, rows, LANES), f32),
        ),
        in_specs=[hbm] * 4,
        out_specs=(vmem, vmem),
        scratch_shapes=[
            planes(steps),
            planes(steps + 1),
            planes(steps + 1),
            planes(steps + 1),
            planes(half + 1),
            planes(half + 1),
            planes(half + 1),
            planes(half),
            planes(steps),
            planes(5),
            planes(2),
            pltpu.VMEM((2, 6, blocks, max(AROUND), LANES), f32),
            pltpu.SemaphoreType.DMA((7,)),
            pltpu.SemaphoreType.DMA,
            pltpu.SemaphoreType.DMA((6, 2)),
            pltpu.SemaphoreType.DMA((2, 6)),
            pltpu.SemaphoreType.DMA((2,)),
            pltpu.SemaphoreType.REGULAR,
            pltpu.SemaphoreType.DMA,
            pltpu.SemaphoreType.DMA((9,)),
        ],
        compiler_params=pltpu.CompilerParams(
            collective_id=0, has_side_effects=True, vmem_limit_bytes=44 * 1024 * 1024
        ),
        name="cycle",
    )(*(pltpu.with_memory_space_constraint(a, pltpu.HBM) for a in (source, guess, start_state, conduct)))
    return pl.pallas_call(
        functools.partial(store_kernel, steps, rows, blocks),
        out_shape=(jax.ShapeDtypeStruct(source.shape, f32), jax.ShapeDtypeStruct(source.shape, f32)),
        in_specs=[vmem, vmem],
        out_specs=(hbm, hbm),
        scratch_shapes=[pltpu.SemaphoreType.DMA((2,))],
        compiler_params=pltpu.CompilerParams(vmem_limit_bytes=16 * 1024 * 1024),
        name="store",
    )(u3, res)


def solution(mesh):
    return jax.shard_map(
        shards,
        mesh=mesh,
        in_specs=(
            P("tm", "space", None),
            P("tm", "space", None),
            P("space", None),
            P("space", None),
        ),
        out_specs=(P("tm", "space", None), P("tm", "space", None)),
        check_vma=False,
    )
```
